32 devices in a mesh: rows: 32 (over z, y, x, core).
Axes of the slice: x: 2, y: 2, z: 4, core: 2. Of those that a mesh axis runs over, the one named last changes fastest.
Arguments:
- p_left: bfloat16 [120, 262144], P(None, 'rows'), may hold values from -0.5 to 0.5
- phi_right: bfloat16 [120, 262144], P(None, 'rows'), may hold values from -0.01171875 to 0.01171875
- v_cols: bfloat16 [40, 262144], P(None, 'rows'), may hold values from -6 to 6
- w_cols: bfloat16 [40, 262144], P(None, 'rows'), may hold values from -6 to 6
- residual: bfloat16 [262144], P('rows'), may hold values from -8 to 8, as said below
Outputs:
- update: float32 [262144], P('rows')
- q_left: bfloat16 [160, 262144], P(None, 'rows')
- q_right: bfloat16 [160, 262144], P(None, 'rows')
- rms_norms: float32 [2], replicated
The draws below stay inside these ranges and needn't reach their ends.
Inputs may be any that keep to these rules, and one draw needn't show every extreme that they name: A residual that lies mostly in the span of the rows of v_cols.
All inputs are finite; a program needn't handle non-finite values.
Results may differ from the reference program's by a relative error of at most 0.0039.
Values may be sent and summed in bfloat16 or wider, within the bound.
No kernel may reach another device: no remote copies, remote signals or barrier semaphores. Data moves between devices by JAX's collectives and lax.ppermute only.
A program may use at most 128 MiB of HBM per device.

```python
import jax
import jax.numpy as jnp
from jax import lax

MDEV = 8192
COLS = 40
RANK = 120
CROSS = 160
MROWS = 262144
N_ROWS = 32


def blended_rows(key, count):
    own = jnp.clip(jax.random.normal(jax.random.fold_in(key, 1), (count, MROWS), jnp.float32), -5.0, 5.0)
    commons = jnp.clip(jax.random.normal(jax.random.fold_in(key, 2), (4, MROWS), jnp.float32), -5.0, 5.0)
    own_share = 0.6
    loads = jax.random.normal(jax.random.fold_in(key, 3), (count, 4), jnp.float32)
    loads = loads / jnp.sqrt(jnp.sum(loads * loads, axis=1, keepdims=True) + 1e-06)
    shared = jnp.dot(loads, commons)
    common_share = jnp.sqrt(1.0 - own_share * own_share)
    return own_share * own + common_share * shared


def paired_columns(key):
    base = jnp.clip(blended_rows(jax.random.fold_in(key, 11), COLS), -6.0, 6.0)
    weights = jnp.clip(jax.random.normal(jax.random.fold_in(key, 12), (COLS,), jnp.float32), -3.0, 3.0)
    noise = jnp.clip(jax.random.normal(jax.random.fold_in(key, 13), (MROWS,), jnp.float32), -6.0, 6.0)
    mixed = jnp.dot(weights, base) / jnp.sqrt(jnp.float32(COLS)) + 0.3 * noise
    mixed = mixed / jnp.sqrt(jnp.mean(mixed * mixed) + 1e-06)
    return (base, jnp.clip(mixed, -8.0, 8.0))


def draw_v_cols(key, part):
    return paired_columns(key)[0].astype(jnp.bfloat16)


def draw_residual(key, part):
    return paired_columns(key)[1].astype(jnp.bfloat16)


def draw_p_left(key, part):
    rows = blended_rows(jax.random.fold_in(key, 21), RANK) / jnp.sqrt(jnp.float32(RANK))
    return jnp.clip(rows, -0.5, 0.5).astype(jnp.bfloat16)


def draw_phi_right(key, part):
    scale = 1.0 / jnp.sqrt(jnp.float32(MROWS))
    rows = blended_rows(jax.random.fold_in(key, 31), RANK) * scale
    return jnp.clip(rows, -6.0 * scale, 6.0 * scale).astype(jnp.bfloat16)


def block_scale(rng, shape, shards, low, high):
    gain = 1.0
    for axis_at, blocks in shards:
        steps = jax.random.uniform(jax.random.fold_in(jax.random.fold_in(rng, 6), axis_at), (blocks,), jnp.float32, low / len(shards), high / len(shards))
        gain = gain * jnp.repeat(jnp.exp(steps), shape[axis_at] // blocks).reshape((-1,) + (1,) * (len(shape) - 1 - axis_at))
    return gain


def centred(key, shape, spread, most, split=(), kind=jnp.bfloat16):
    loudness = block_scale(key, shape, split, -0.22, 0.18) if split else 1.0
    values = jax.random.normal(key, shape, jnp.float32) * spread * loudness
    return jnp.minimum(jnp.maximum(values, -most), most).astype(kind)


def setup_inputs(seed: int = 0) -> dict:
    keys = jax.random.split(jax.random.key(seed), 6)
    return {
        "p_left": draw_p_left(jax.random.fold_in(keys[5], 71), 0),
        "phi_right": draw_phi_right(jax.random.fold_in(keys[5], 71), 0),
        "v_cols": draw_v_cols(jax.random.fold_in(keys[5], 71), 0),
        "w_cols": centred(keys[3], (COLS, MROWS), 1.0, 6.0, ((1, 32),)),
        "residual": draw_residual(jax.random.fold_in(keys[5], 71), 0),
    }


def lower_solve(factor, rhs, transposed=False):
    return lax.linalg.triangular_solve(factor, rhs, left_side=True, lower=True, transpose_a=transposed)

def split_blocks(array):
    return array.reshape(array.shape[0], N_ROWS, MDEV).transpose(1, 0, 2)

def reference(p_left, phi_right, v_cols, w_cols, residual):
    single = jnp.float32
    half = jnp.bfloat16
    highest = lax.Precision.HIGHEST
    col_gram = jnp.dot(v_cols, v_cols.T, preferred_element_type=single)
    col_res = jnp.dot(v_cols, residual, preferred_element_type=single)
    phi_cols = jnp.dot(phi_right, v_cols.T, preferred_element_type=single)
    phi_res = jnp.dot(phi_right, residual, preferred_element_type=single)
    res_sq = jnp.dot(residual, residual, preferred_element_type=single)
    col_chol = jnp.linalg.cholesky(col_gram)
    coeffs = -lower_solve(col_chol, lower_solve(col_chol, col_res[:, None]), True)[:, 0]
    mix_half = phi_cols.astype(half)
    res_half = phi_res.astype(half)

    def section(pieces):
        p_blk, phi_blk, v_blk, w_blk = pieces
        w_tilde = w_blk.astype(single) - jnp.dot(mix_half.T, p_blk, preferred_element_type=single)
        upd = jnp.dot(coeffs, w_tilde, precision=highest) - jnp.dot(res_half, p_blk, preferred_element_type=single)
        left = jnp.concatenate([p_blk.astype(single), lower_solve(col_chol, w_tilde)], 0)
        right = jnp.concatenate([phi_blk.astype(single), lower_solve(col_chol, v_blk.astype(single))], 0)
        return (upd, left, right)
    blocks = (split_blocks(p_left), split_blocks(phi_right), split_blocks(v_cols), split_blocks(w_cols))

    def first_pass(carry, pieces):
        upd, left, right = section(pieces)
        left_acc = carry[0] + jnp.dot(left, left.T, precision=highest)
        right_acc = carry[1] + jnp.dot(right, right.T, precision=highest)
        upd_acc = carry[2] + jnp.sum(upd * upd)
        return ((left_acc, right_acc, upd_acc), upd)
    start = (jnp.zeros((CROSS, CROSS), single), jnp.zeros((CROSS, CROSS), single), jnp.zeros((), single))
    (left_gram, right_gram, upd_sq), upd_blocks = lax.scan(first_pass, start, blocks)
    left_chol = jnp.linalg.cholesky(left_gram)
    right_chol = jnp.linalg.cholesky(right_gram)

    def second_pass(pieces):
        upd, left, right = section(pieces)
        return (lower_solve(left_chol, left).astype(half), lower_solve(right_chol, right).astype(half))
    left_blocks, right_blocks = lax.map(second_pass, blocks)
    update = upd_blocks.reshape(MROWS)
    q_right = right_blocks.transpose(1, 0, 2).reshape(CROSS, MROWS)
    left_full = left_blocks.transpose(1, 0, 2).reshape(CROSS, MROWS)
    q_left = left_full.reshape(CROSS, MDEV, N_ROWS).transpose(0, 2, 1).reshape(CROSS, MROWS)
    rms_norms = jnp.sqrt(jnp.stack([res_sq, upd_sq]) / MROWS)
    return (update, q_left, q_right, rms_norms)
```

```python
import functools

import jax
import jax.numpy as jnp
from jax import lax
from jax.experimental import pallas as pl
from jax.experimental.pallas import tpu as pltpu
from jax.sharding import PartitionSpec as P

SINGLE = jnp.float32
HALF = jnp.bfloat16
LANES = 128
BLOCK = 8
HIGHEST = lax.Precision.HIGHEST
NT = (((1,), (1,)), ((), ()))
TN = (((0,), (0,)), ((), ()))
VMEM_LIMIT = 56 * 1024 * 1024


def iota(shape, dim):
    return lax.broadcasted_iota(jnp.int32, shape, dim)


def dot_hi(a, b, dims=None):
    if dims is None:
        return jnp.dot(a, b, precision=HIGHEST, preferred_element_type=SINGLE)
    return lax.dot_general(a, b, dims, precision=HIGHEST, preferred_element_type=SINGLE)


def to_half(x):
    return x.astype(HALF).astype(SINGLE)


def sort_kernel(n, p_ref, w_ref, out_ref, turned, turned_rest):
    cross, take = out_ref.shape[1:]
    rest = cross - LANES
    step = 512
    for at in range(0, p_ref.shape[1], step):
        both = jnp.concatenate(
            [p_ref[:, at : at + step].astype(SINGLE), w_ref[:, at : at + step].astype(SINGLE)], 0
        )
        turned[at : at + step, :] = both[0:LANES].T
        turned_rest[at : at + step, 0:rest] = both[LANES:cross].T
    for owner in range(n):
        mine = pl.ds(owner, take, stride=n)
        out_ref[owner, 0:LANES, :] = turned[mine, :].T.astype(HALF)
        out_ref[owner, LANES:cross, :] = turned_rest[mine, :].T[0:rest].astype(HALF)


def sort_by_owner(p_left, w_cols, n):
    rank, local = p_left.shape
    cols = w_cols.shape[0]
    share = local // n
    chunks = share // LANES if share % LANES == 0 else 1
    wide = local // chunks
    return pl.pallas_call(
        functools.partial(sort_kernel, n),
        grid=(chunks,),
        in_specs=[
            pl.BlockSpec((rank, wide), lambda i: (0, i)),
            pl.BlockSpec((cols, wide), lambda i: (0, i)),
        ],
        out_specs=pl.BlockSpec((n, rank + cols, share // chunks), lambda i: (0, 0, i)),
        out_shape=jax.ShapeDtypeStruct((n, rank + cols, share), HALF),
        scratch_shapes=[pltpu.VMEM((wide, LANES), SINGLE), pltpu.VMEM((wide, LANES), SINGLE)],
        compiler_params=pltpu.CompilerParams(vmem_limit_bytes=VMEM_LIMIT),
        name="sort_by_owner",
    )(p_left, w_cols)


def gram_kernel(p_ref, w_ref, phi_ref, v_ref, res_ref, out_ref, left, right):
    at = pl.program_id(0)

    @pl.when(at == 0)
    def _():
        left[...] = jnp.zeros_like(left)
        right[...] = jnp.zeros_like(right)

    x = jnp.concatenate([p_ref[...].astype(SINGLE), w_ref[...].astype(SINGLE)], 0).astype(HALF)
    left[...] += lax.dot_general(x, x, NT, preferred_element_type=SINGLE)
    wide = res_ref.shape[1]
    last = jnp.where(iota((8, wide), 0) == 0, res_ref[...].astype(SINGLE), 0.0)
    y = jnp.concatenate([phi_ref[...].astype(SINGLE), v_ref[...].astype(SINGLE), last], 0).astype(HALF)
    right[...] += lax.dot_general(y, y, NT, preferred_element_type=SINGLE)

    @pl.when(at == pl.num_programs(0) - 1)
    def _():
        cross = left.shape[0]
        m = LANES
        e = cross - m
        rows, lanes = iota((m, m), 0), iota((m, m), 1)
        top_right = right[0:m, 0:m]
        out_ref[0:m, :] = jnp.where(lanes <= rows, left[0:m, 0:m], top_right)
        out_ref[m : m + e, :] = left[m:cross, 0:m]
        out_ref[m + e : m + 2 * e, :] = right[m:cross, 0:m]
        out_ref[m + 2 * e : m + 3 * e, :] = jnp.zeros((e, m), SINGLE)
        out_ref[m + 2 * e : m + 3 * e, 0:e] = left[m:cross, m:cross]
        out_ref[m + 2 * e : m + 3 * e, e : 2 * e] = right[m:cross, m:cross]
        base = m + 3 * e
        out_ref[base : base + 8, :] = jnp.zeros((8, m), SINGLE)
        out_ref[base : base + 1, :] = jnp.sum(jnp.where(rows == lanes, top_right, 0.0), 0, keepdims=True)
        out_ref[base + 1 : base + 2, :] = right[cross : cross + 1, 0:m]
        out_ref[base + 2 : base + 3, 0 : e + 1] = right[cross : cross + 1, m : cross + 1]


def packed_rows(cross):
    return LANES + 3 * (cross - LANES) + 8


def packed_grams(p_left, w_cols, phi_right, v_cols, residual):
    rank, local = p_left.shape
    cols = w_cols.shape[0]
    cross = rank + cols
    wide = min(local, 2048)
    spec = lambda rows: pl.BlockSpec((rows, wide), lambda i: (0, i))
    return pl.pallas_call(
        gram_kernel,
        grid=(local // wide,),
        in_specs=[spec(rank), spec(cols), spec(rank), spec(cols), spec(1)],
        out_specs=pl.BlockSpec((packed_rows(cross), LANES), lambda i: (0, 0)),
        out_shape=jax.ShapeDtypeStruct((packed_rows(cross), LANES), SINGLE),
        scratch_shapes=[pltpu.VMEM((cross, cross), SINGLE), pltpu.VMEM((cross + 8, cross + 8), SINGLE)],
        compiler_params=pltpu.CompilerParams(vmem_limit_bytes=VMEM_LIMIT),
        name="packed_grams",
    )(p_left, w_cols, phi_right, v_cols, residual.reshape(1, local))


def eliminate(refs, tops, k):
    panels = []
    for ref, top in zip(refs, tops):
        cross = ref.shape[1]
        x = ref[pl.ds(pl.multiple_of(k - top, BLOCK), BLOCK), :]
        lane, sub = iota((BLOCK, cross), 1), iota((BLOCK, cross), 0)
        column = [
            jnp.sum(jnp.where(lane == k + i, x, 0.0), 1, keepdims=True) for i in range(BLOCK)
        ]
        rel = lane - k
        x = jnp.where((rel >= 0) & (rel < BLOCK), jnp.where(rel == sub, 1.0, 0.0), x)
        panels.append([x, column, rel, sub])
    thin = iota((BLOCK, 1), 0)
    for i in range(BLOCK):
        for panel in panels:
            x, column, rel, sub = panel
            scale = lax.rsqrt(column[i][i : i + 1, :])
            factor = jnp.where(thin > i, column[i] * scale, 0.0)
            for j in range(i + 1, BLOCK):
                column[j] = column[j] - factor * (column[j][i : i + 1, :] * scale)
            row = x[i : i + 1, :] * scale
            panel[0] = jnp.where(sub == i, row, x - factor * row)
    for ref, top, (x, _, rel, _) in zip(refs, tops, panels):
        cross = ref.shape[1]
        right = jnp.where(rel >= BLOCK, x, 0.0)
        done = jnp.where(rel < BLOCK, x, 0.0)
        r0 = to_half(right)
        r1 = to_half(right - r0)
        r2 = right - r0 - r1
        x0 = to_half(x)
        x1 = to_half(x - x0)
        x2 = x - x0 - x1
        lhs = jnp.concatenate([r0, r0, r0, r1, r1, r2], 0)
        if top:
            lhs = jnp.concatenate([lhs, jnp.zeros((LANES - lhs.shape[0], cross), SINGLE)], 0)
            lhs = lhs.T[top:cross, 0 : 6 * BLOCK].astype(HALF)
        else:
            lhs = lhs.T.astype(HALF)
        rhs = jnp.concatenate([x0, x1, x2, x0, x1, x0], 0).astype(HALF)
        change = jnp.dot(lhs, rhs, preferred_element_type=SINGLE)
        here = iota(ref.shape, 1) - k
        ref[...] = jnp.where((here >= 0) & (here < BLOCK), 0.0, ref[...]) - change
        ref[pl.ds(pl.multiple_of(k - top, BLOCK), BLOCK), :] = done


def small_kernel(rank, count, g_ref, kl_ref, kr_ref, u_ref, rms_ref, left, right, tail):
    cross = left.shape[0]
    m = LANES
    e = cross - m
    base = m + 3 * e
    rows, lanes = iota((m, m), 0), iota((m, m), 1)
    top = g_ref[0:m, :]
    lower = jnp.where(lanes < rows, top, 0.0)
    upper = jnp.where(lanes > rows, top, 0.0)
    same = rows == lanes
    left[0:m, 0:m] = lower + lower.T + jnp.where(same, top, 0.0)
    right[0:m, 0:m] = upper + upper.T + jnp.where(same, g_ref[base : base + 1, :], 0.0)
    left[m:cross, 0:m] = g_ref[m : m + e, :]
    right[m:cross, 0:m] = g_ref[m + e : m + 2 * e, :]
    left[0:m, m:cross] = g_ref[m : m + e, :].T
    right[0:m, m:cross] = g_ref[m + e : m + 2 * e, :].T
    left[m:cross, m:cross] = g_ref[m + 2 * e : m + 3 * e, 0:e]
    right[m:cross, m:cross] = g_ref[m + 2 * e : m + 3 * e, e : 2 * e]
    g_left = left[...]
    g_right = right[...]
    res_first = g_ref[base + 1 : base + 2, :]
    res_rest = g_ref[base + 2 : base + 3, 0:e]
    res_row = jnp.concatenate([res_first, res_rest], 1)
    res_sq = g_ref[base + 2 : base + 3, e : e + 1]

    tail[...] = g_right[rank:cross, :]
    lax.fori_loop(
        rank // BLOCK, cross // BLOCK, lambda b, c: (eliminate([tail], [rank], b * BLOCK), c)[1], 0
    )
    low_lane = iota((cross - rank, cross), 1)
    low_row = iota((cross - rank, cross), 0)
    inverse = jnp.where(low_lane >= rank, tail[...], 0.0)
    eye = jnp.where(iota((rank, cross), 0) == iota((rank, cross), 1), 1.0, 0.0)

    mix = jnp.where(
        low_lane < rank, -to_half(g_right[rank:cross, :]), jnp.where(low_lane == low_row + rank, 1.0, 0.0)
    )
    to_tilde = jnp.concatenate([eye, mix], 0)
    t_right = jnp.concatenate([eye, inverse], 0)
    t_left = jnp.concatenate([eye, dot_hi(inverse, to_tilde)], 0)

    lane8 = iota((BLOCK, cross), 1)
    res8 = jnp.broadcast_to(res_row, (BLOCK, cross))
    half_way = dot_hi(jnp.where(lane8 >= rank, res8, 0.0), inverse, NT)
    coeffs = -dot_hi(half_way, inverse)
    u = dot_hi(jnp.where(lane8 < rank, -to_half(res8), coeffs), to_tilde)
    upd_sq = jnp.sum(dot_hi(u, g_left) * u, 1, keepdims=True)[0:1, :]
    u0 = to_half(u)
    u1 = to_half(u - u0)
    u2 = u - u0 - u1
    sub8 = iota((BLOCK, cross), 0)
    u_ref[...] = jnp.where(sub8 == 0, u0, jnp.where(sub8 == 1, u1, jnp.where(sub8 == 2, u2, 0.0)))
    lane_out = iota((1, LANES), 1)
    rms_ref[...] = jnp.sqrt(jnp.where(lane_out == 0, res_sq, upd_sq) / count)

    left[...] = dot_hi(dot_hi(t_left, g_left), t_left, NT)
    right[...] = dot_hi(dot_hi(t_right, g_right), t_right, NT)
    lax.fori_loop(
        0, cross // BLOCK, lambda b, c: (eliminate([left, right], [0, 0], b * BLOCK), c)[1], 0
    )
    for source, turn, out in ((left, t_left, kl_ref), (right, t_right, kr_ref)):
        k = dot_hi(source[...], turn)
        k0 = to_half(k)
        out[0:cross, :] = k0.astype(HALF)
        out[cross : 2 * cross, :] = (k - k0).astype(HALF)


def small_algebra(packed, rank, cols, count):
    cross = rank + cols
    vmem = pl.BlockSpec(memory_space=pltpu.VMEM)
    return pl.pallas_call(
        functools.partial(small_kernel, rank, count),
        in_specs=[vmem],
        out_specs=[vmem] * 4,
        out_shape=[
            jax.ShapeDtypeStruct((2 * cross, cross), HALF),
            jax.ShapeDtypeStruct((2 * cross, cross), HALF),
            jax.ShapeDtypeStruct((BLOCK, cross), SINGLE),
            jax.ShapeDtypeStruct((1, LANES), SINGLE),
        ],
        scratch_shapes=[
            pltpu.VMEM((cross, cross), SINGLE),
            pltpu.VMEM((cross, cross), SINGLE),
            pltpu.VMEM((cols, cross), SINGLE),
        ],
        compiler_params=pltpu.CompilerParams(vmem_limit_bytes=VMEM_LIMIT),
        name="small_algebra",
    )(packed)


def right_kernel(p_ref, w_ref, phi_ref, v_ref, k_ref, u_ref, upd_ref, q_ref):
    cross = k_ref.shape[1]
    y = jnp.concatenate([phi_ref[...].astype(SINGLE), v_ref[...].astype(SINGLE)], 0).astype(HALF)
    both = jnp.dot(k_ref[...], y, preferred_element_type=SINGLE)
    q_ref[...] = (both[0:cross] + both[cross : 2 * cross]).astype(HALF)
    x = jnp.concatenate([p_ref[...].astype(SINGLE), w_ref[...].astype(SINGLE)], 0).astype(HALF)
    upd_ref[...] = jnp.sum(
        jnp.dot(u_ref[...].astype(HALF), x, preferred_element_type=SINGLE), 0, keepdims=True
    )


def right_products(p_left, w_cols, phi_right, v_cols, k_right, u):
    rank, local = p_left.shape
    cols = w_cols.shape[0]
    cross = rank + cols
    wide = min(local, 2048)
    spec = lambda rows: pl.BlockSpec((rows, wide), lambda i: (0, i))
    return pl.pallas_call(
        right_kernel,
        grid=(local // wide,),
        in_specs=[
            spec(rank), spec(cols), spec(rank), spec(cols),
            pl.BlockSpec((2 * cross, cross), lambda i: (0, 0)),
            pl.BlockSpec((BLOCK, cross), lambda i: (0, 0)),
        ],
        out_specs=[spec(1), spec(cross)],
        out_shape=[
            jax.ShapeDtypeStruct((1, local), SINGLE),
            jax.ShapeDtypeStruct((cross, local), HALF),
        ],
        compiler_params=pltpu.CompilerParams(vmem_limit_bytes=VMEM_LIMIT),
        name="right_products",
    )(p_left, w_cols, phi_right, v_cols, k_right, u)


def left_kernel(x_ref, k_ref, q_ref):
    group, cross, share = x_ref.shape
    for i in range(group):
        both = jnp.dot(k_ref[...], x_ref[i], preferred_element_type=SINGLE)
        q_ref[:, i * share : (i + 1) * share] = (both[0:cross] + both[cross : 2 * cross]).astype(HALF)


def left_products(sorted_x, k_left):
    n, cross, share = sorted_x.shape
    group = max(1, 2048 // share)
    return pl.pallas_call(
        left_kernel,
        grid=(n // group,),
        in_specs=[
            pl.BlockSpec((group, cross, share), lambda i: (i, 0, 0)),
            pl.BlockSpec((2 * cross, cross), lambda i: (0, 0)),
        ],
        out_specs=pl.BlockSpec((cross, group * share), lambda i: (0, i)),
        out_shape=jax.ShapeDtypeStruct((cross, n * share), HALF),
        compiler_params=pltpu.CompilerParams(vmem_limit_bytes=VMEM_LIMIT),
        name="left_products",
    )(sorted_x, k_left)


def sum_over_rows(x):
    n = lax.axis_size("rows")
    reach = 1
    while reach < n:
        x = x + lax.ppermute(x, "rows", [(i, i ^ reach) for i in range(n)])
        reach *= 2
    return x


def shards(p_left, phi_right, v_cols, w_cols, residual):
    rank, local = p_left.shape
    cols = v_cols.shape[0]
    n = lax.axis_size("rows")
    mine = sort_by_owner(p_left, w_cols, n)
    owned = lax.all_to_all(mine, "rows", split_axis=0, concat_axis=0, tiled=True)
    packed = sum_over_rows(packed_grams(p_left, w_cols, phi_right, v_cols, residual))
    k_left, k_right, u, rms = small_algebra(packed, rank, cols, float(local * n))
    update, q_right = right_products(p_left, w_cols, phi_right, v_cols, k_right, u)
    q_left = left_products(owned, k_left)
    return (update.reshape(local), q_left, q_right, rms[0, 0:2])


def solution(mesh):
    placed = (P(None, "rows"), P(None, "rows"), P(None, "rows"), P(None, "rows"), P("rows"))
    return jax.shard_map(
        shards,
        mesh=mesh,
        in_specs=placed,
        out_specs=(P("rows"), P(None, "rows"), P(None, "rows"), P()),
        check_vma=False,
    )
```

```python
import functools

import jax
import jax.numpy as jnp
from jax import lax
from jax.experimental import pallas as pl
from jax.experimental.pallas import tpu as pltpu
from jax.sharding import PartitionSpec as P

SINGLE = jnp.float32
HALF = jnp.bfloat16
LANES = 128
BLOCK = 8
HIGHEST = lax.Precision.HIGHEST
NT = (((1,), (1,)), ((), ()))
TN = (((0,), (0,)), ((), ()))
VMEM_LIMIT = 24 * 1024 * 1024
SORT_TILE = 256


def iota(shape, dim):
    return lax.broadcasted_iota(jnp.int32, shape, dim)


def dot_hi(a, b, dims=None):
    if dims is None:
        return jnp.dot(a, b, precision=HIGHEST, preferred_element_type=SINGLE)
    return lax.dot_general(a, b, dims, precision=HIGHEST, preferred_element_type=SINGLE)


def in_vmem(x):
    return pltpu.with_memory_space_constraint(x, pltpu.VMEM)


def in_hbm(*xs):
    return [pltpu.with_memory_space_constraint(x, pltpu.HBM) for x in xs]


def to_half(x):
    return x.astype(HALF).astype(SINGLE)


def sort_kernel(n, p_ref, w_ref, out_ref, turned):
    cross = out_ref.shape[1]
    wide = p_ref.shape[1]
    tile = SORT_TILE
    runs = tile // n
    row, column = iota((tile, tile), 0), iota((tile, tile), 1)
    wanted = lax.rem(row, runs) * n + lax.div(row, runs)
    permutation = jnp.where(column == wanted, 1.0, 0.0).astype(HALF)
    eye = jnp.where(iota((cross, cross), 0) == iota((cross, cross), 1), 1.0, 0.0).astype(HALF)
    pair = 16 // runs if runs < 16 else 1
    for at in range(0, wide, tile * pair):
        parts = []
        for i in range(pair):
            cut = slice(at + i * tile, at + (i + 1) * tile)
            both = jnp.concatenate([p_ref[:, cut].astype(SINGLE), w_ref[:, cut].astype(SINGLE)], 0)
            part = lax.dot_general(permutation, both.astype(HALF), NT, preferred_element_type=SINGLE)
            parts.append(part.reshape(n, runs, cross))
        rows = slice(at // n, at // n + runs * pair)
        turned[:, rows, :] = jnp.concatenate(parts, 1).astype(HALF)
    for owner in range(n):
        mine = lax.dot_general(eye, turned[owner], NT, preferred_element_type=SINGLE)
        out_ref[owner] = mine.astype(HALF)


def sort_by_owner(p_left, w_cols, n):
    rank, local = p_left.shape
    cols = w_cols.shape[0]
    share = local // n
    chunks = share // LANES if share % LANES == 0 else 1
    wide = local // chunks
    return pl.pallas_call(
        functools.partial(sort_kernel, n),
        grid=(chunks,),
        in_specs=[
            pl.BlockSpec((rank, wide), lambda i: (0, i)),
            pl.BlockSpec((cols, wide), lambda i: (0, i)),
        ],
        out_specs=pl.BlockSpec((n, rank + cols, share // chunks), lambda i: (0, 0, i)),
        out_shape=pltpu.HBM((n, rank + cols, share), HALF),
        scratch_shapes=[pltpu.VMEM((n, share // chunks, rank + cols), HALF)],
        compiler_params=pltpu.CompilerParams(vmem_limit_bytes=VMEM_LIMIT),
        name="sort_by_owner",
    )(*in_hbm(p_left, w_cols))


def gram_kernel(p_ref, w_ref, phi_ref, v_ref, res_ref, out_ref, left, right):
    at = pl.program_id(0)

    @pl.when(at == 0)
    def _():
        left[...] = jnp.zeros_like(left)
        right[...] = jnp.zeros_like(right)

    x = jnp.concatenate([p_ref[...].astype(SINGLE), w_ref[...].astype(SINGLE)], 0).astype(HALF)
    left[...] += lax.dot_general(x, x, NT, preferred_element_type=SINGLE)
    wide = res_ref.shape[1]
    last = jnp.where(iota((8, wide), 0) == 0, res_ref[...].astype(SINGLE), 0.0)
    y = jnp.concatenate([phi_ref[...].astype(SINGLE), v_ref[...].astype(SINGLE), last], 0).astype(HALF)
    right[...] += lax.dot_general(y, y, NT, preferred_element_type=SINGLE)

    @pl.when(at == pl.num_programs(0) - 1)
    def _():
        cross = left.shape[0]
        m = LANES
        e = cross - m
        rows, lanes = iota((m, m), 0), iota((m, m), 1)
        top_right = right[0:m, 0:m]
        out_ref[0:m, :] = jnp.where(lanes <= rows, left[0:m, 0:m], top_right)
        out_ref[m : m + e, :] = left[m:cross, 0:m]
        out_ref[m + e : m + 2 * e, :] = right[m:cross, 0:m]
        out_ref[m + 2 * e : m + 3 * e, :] = jnp.zeros((e, m), SINGLE)
        out_ref[m + 2 * e : m + 3 * e, 0:e] = left[m:cross, m:cross]
        out_ref[m + 2 * e : m + 3 * e, e : 2 * e] = right[m:cross, m:cross]
        base = m + 3 * e
        out_ref[base:, :] = jnp.zeros((out_ref.shape[0] - base, m), SINGLE)
        out_ref[base : base + 1, :] = jnp.sum(jnp.where(rows == lanes, top_right, 0.0), 0, keepdims=True)
        out_ref[base + 1 : base + 2, :] = right[cross : cross + 1, 0:m]
        out_ref[base + 2 : base + 3, 0 : e + 1] = right[cross : cross + 1, m : cross + 1]


def packed_rows(cross):
    used = LANES + 3 * (cross - LANES) + BLOCK
    return -(-used // (8 * BLOCK)) * 8 * BLOCK


def packed_grams(p_left, w_cols, phi_right, v_cols, residual):
    rank, local = p_left.shape
    cols = w_cols.shape[0]
    cross = rank + cols
    wide = min(local, 2048)
    spec = lambda rows: pl.BlockSpec((rows, wide), lambda i: (0, i))
    return pl.pallas_call(
        gram_kernel,
        grid=(local // wide,),
        in_specs=[spec(rank), spec(cols), spec(rank), spec(cols), spec(1)],
        out_specs=pl.BlockSpec((packed_rows(cross), LANES), lambda i: (0, 0)),
        out_shape=pltpu.VMEM((packed_rows(cross), LANES), SINGLE),
        scratch_shapes=[pltpu.VMEM((cross, cross), SINGLE), pltpu.VMEM((cross + 8, cross + 8), SINGLE)],
        compiler_params=pltpu.CompilerParams(vmem_limit_bytes=VMEM_LIMIT),
        name="packed_grams",
    )(*in_hbm(p_left, w_cols, phi_right, v_cols), residual.reshape(1, local))


def eliminate(refs, tops, k):
    panels = []
    for ref, top in zip(refs, tops):
        cross = ref.shape[1]
        x = ref[pl.ds(pl.multiple_of(k - top, BLOCK), BLOCK), :]
        lane, sub = iota((BLOCK, cross), 1), iota((BLOCK, cross), 0)
        column = [
            jnp.sum(jnp.where(lane == k + i, x, 0.0), 1, keepdims=True) for i in range(BLOCK)
        ]
        rel = lane - k
        x = jnp.where((rel >= 0) & (rel < BLOCK), jnp.where(rel == sub, 1.0, 0.0), x)
        panels.append([x, column, rel, sub])
    thin = iota((BLOCK, 1), 0)
    for i in range(BLOCK):
        for panel in panels:
            x, column, rel, sub = panel
            scale = lax.rsqrt(column[i][i : i + 1, :])
            factor = jnp.where(thin > i, column[i] * scale, 0.0)
            for j in range(i + 1, BLOCK):
                column[j] = column[j] - factor * (column[j][i : i + 1, :] * scale)
            row = x[i : i + 1, :] * scale
            panel[0] = jnp.where(sub == i, row, x - factor * row)
    for ref, top, (x, _, rel, _) in zip(refs, tops, panels):
        cross = ref.shape[1]
        right = jnp.where(rel >= BLOCK, x, 0.0)
        done = jnp.where(rel < BLOCK, x, 0.0)
        r0 = to_half(right)
        r1 = to_half(right - r0)
        r2 = right - r0 - r1
        x0 = to_half(x)
        x1 = to_half(x - x0)
        x2 = x - x0 - x1
        lhs = jnp.concatenate([r0, r0, r0, r1, r1, r2], 0)
        if top:
            lhs = jnp.concatenate([lhs, jnp.zeros((LANES - lhs.shape[0], cross), SINGLE)], 0)
            lhs = lhs.T[top:cross, 0 : 6 * BLOCK].astype(HALF)
        else:
            lhs = lhs.T.astype(HALF)
        rhs = jnp.concatenate([x0, x1, x2, x0, x1, x0], 0).astype(HALF)
        change = jnp.dot(lhs, rhs, preferred_element_type=SINGLE)
        here = iota(ref.shape, 1) - k
        ref[...] = jnp.where((here >= 0) & (here < BLOCK), 0.0, ref[...]) - change
        ref[pl.ds(pl.multiple_of(k - top, BLOCK), BLOCK), :] = done


def small_kernel(rank, count, g_ref, kl_ref, kr_ref, u_ref, rms_ref, left, right, tail):
    cross = left.shape[0]
    m = LANES
    e = cross - m
    base = m + 3 * e
    rows, lanes = iota((m, m), 0), iota((m, m), 1)
    top = g_ref[0:m, :]
    lower = jnp.where(lanes < rows, top, 0.0)
    upper = jnp.where(lanes > rows, top, 0.0)
    same = rows == lanes
    left[0:m, 0:m] = lower + lower.T + jnp.where(same, top, 0.0)
    right[0:m, 0:m] = upper + upper.T + jnp.where(same, g_ref[base : base + 1, :], 0.0)
    left[m:cross, 0:m] = g_ref[m : m + e, :]
    right[m:cross, 0:m] = g_ref[m + e : m + 2 * e, :]
    left[0:m, m:cross] = g_ref[m : m + e, :].T
    right[0:m, m:cross] = g_ref[m + e : m + 2 * e, :].T
    left[m:cross, m:cross] = g_ref[m + 2 * e : m + 3 * e, 0:e]
    right[m:cross, m:cross] = g_ref[m + 2 * e : m + 3 * e, e : 2 * e]
    g_left = left[...]
    g_right = right[...]
    res_first = g_ref[base + 1 : base + 2, :]
    res_rest = g_ref[base + 2 : base + 3, 0:e]
    res_row = jnp.concatenate([res_first, res_rest], 1)
    res_sq = g_ref[base + 2 : base + 3, e : e + 1]

    tail[...] = g_right[rank:cross, :]
    lax.fori_loop(
        rank // BLOCK, cross // BLOCK, lambda b, c: (eliminate([tail], [rank], b * BLOCK), c)[1], 0
    )
    low_lane = iota((cross - rank, cross), 1)
    low_row = iota((cross - rank, cross), 0)
    inverse = jnp.where(low_lane >= rank, tail[...], 0.0)
    eye = jnp.where(iota((rank, cross), 0) == iota((rank, cross), 1), 1.0, 0.0)

    mix = jnp.where(
        low_lane < rank, -to_half(g_right[rank:cross, :]), jnp.where(low_lane == low_row + rank, 1.0, 0.0)
    )
    to_tilde = jnp.concatenate([eye, mix], 0)
    t_right = jnp.concatenate([eye, inverse], 0)
    t_left = jnp.concatenate([eye, dot_hi(inverse, to_tilde)], 0)

    lane8 = iota((BLOCK, cross), 1)
    res8 = jnp.broadcast_to(res_row, (BLOCK, cross))
    half_way = dot_hi(jnp.where(lane8 >= rank, res8, 0.0), inverse, NT)
    coeffs = -dot_hi(half_way, inverse)
    u = dot_hi(jnp.where(lane8 < rank, -to_half(res8), coeffs), to_tilde)
    upd_sq = jnp.sum(dot_hi(u, g_left) * u, 1, keepdims=True)[0:1, :]
    u0 = to_half(u)
    u1 = to_half(u - u0)
    u2 = u - u0 - u1
    sub8 = iota((BLOCK, cross), 0)
    u_ref[...] = jnp.where(sub8 == 0, u0, jnp.where(sub8 == 1, u1, jnp.where(sub8 == 2, u2, 0.0)))
    lane_out = iota((1, LANES), 1)
    rms_ref[...] = jnp.sqrt(jnp.where(lane_out == 0, res_sq, upd_sq) / count)

    left[...] = dot_hi(dot_hi(t_left, g_left), t_left, NT)
    right[...] = dot_hi(dot_hi(t_right, g_right), t_right, NT)
    lax.fori_loop(
        0, cross // BLOCK, lambda b, c: (eliminate([left, right], [0, 0], b * BLOCK), c)[1], 0
    )
    for source, turn, out in ((left, t_left, kl_ref), (right, t_right, kr_ref)):
        k = dot_hi(source[...], turn)
        k0 = to_half(k)
        out[0:cross, :] = k0.astype(HALF)
        out[cross : 2 * cross, :] = (k - k0).astype(HALF)


def small_algebra(packed, rank, cols, count):
    cross = rank + cols
    vmem = pl.BlockSpec(memory_space=pltpu.VMEM)
    return pl.pallas_call(
        functools.partial(small_kernel, rank, count),
        in_specs=[vmem],
        out_specs=[vmem] * 4,
        out_shape=[
            pltpu.VMEM((2 * cross, cross), HALF),
            pltpu.VMEM((2 * cross, cross), HALF),
            pltpu.VMEM((BLOCK, cross), SINGLE),
            jax.ShapeDtypeStruct((1, LANES), SINGLE),
        ],
        scratch_shapes=[
            pltpu.VMEM((cross, cross), SINGLE),
            pltpu.VMEM((cross, cross), SINGLE),
            pltpu.VMEM((cols, cross), SINGLE),
        ],
        compiler_params=pltpu.CompilerParams(vmem_limit_bytes=VMEM_LIMIT),
        name="small_algebra",
    )(in_vmem(packed))


def right_kernel(p_ref, w_ref, phi_ref, v_ref, k_ref, u_ref, upd_ref, q_ref):
    cross = k_ref.shape[1]
    y = jnp.concatenate([phi_ref[...].astype(SINGLE), v_ref[...].astype(SINGLE)], 0).astype(HALF)
    both = jnp.dot(k_ref[...], y, preferred_element_type=SINGLE)
    q_ref[...] = (both[0:cross] + both[cross : 2 * cross]).astype(HALF)
    x = jnp.concatenate([p_ref[...].astype(SINGLE), w_ref[...].astype(SINGLE)], 0).astype(HALF)
    upd_ref[...] = jnp.sum(
        jnp.dot(u_ref[...].astype(HALF), x, preferred_element_type=SINGLE), 0, keepdims=True
    )


def right_products(p_left, w_cols, phi_right, v_cols, k_right, u):
    rank, local = p_left.shape
    cols = w_cols.shape[0]
    cross = rank + cols
    wide = min(local, 2048)
    spec = lambda rows: pl.BlockSpec((rows, wide), lambda i: (0, i))
    return pl.pallas_call(
        right_kernel,
        grid=(local // wide,),
        in_specs=[
            spec(rank), spec(cols), spec(rank), spec(cols),
            pl.BlockSpec((2 * cross, cross), lambda i: (0, 0)),
            pl.BlockSpec((BLOCK, cross), lambda i: (0, 0)),
        ],
        out_specs=[spec(1), spec(cross)],
        out_shape=[
            jax.ShapeDtypeStruct((1, local), SINGLE),
            jax.ShapeDtypeStruct((cross, local), HALF),
        ],
        compiler_params=pltpu.CompilerParams(vmem_limit_bytes=VMEM_LIMIT),
        name="right_products",
    )(*in_hbm(p_left, w_cols, phi_right, v_cols), in_vmem(k_right), in_vmem(u))


def left_kernel(x_ref, k_ref, q_ref):
    group, cross, share = x_ref.shape
    for i in range(group):
        both = jnp.dot(k_ref[...], x_ref[i], preferred_element_type=SINGLE)
        q_ref[:, i * share : (i + 1) * share] = (both[0:cross] + both[cross : 2 * cross]).astype(HALF)


def left_products(sorted_x, k_left):
    n, cross, share = sorted_x.shape
    group = max(1, 2048 // share)
    return pl.pallas_call(
        left_kernel,
        grid=(n // group,),
        in_specs=[
            pl.BlockSpec((group, cross, share), lambda i: (i, 0, 0)),
            pl.BlockSpec((2 * cross, cross), lambda i: (0, 0)),
        ],
        out_specs=pl.BlockSpec((cross, group * share), lambda i: (0, i)),
        out_shape=jax.ShapeDtypeStruct((cross, n * share), HALF),
        compiler_params=pltpu.CompilerParams(vmem_limit_bytes=VMEM_LIMIT),
        name="left_products",
    )(in_vmem(sorted_x), in_vmem(k_left))


def sum_over_rows(x):
    n = lax.axis_size("rows")
    me = lax.axis_index("rows")

    def swap(y, reach):
        return lax.ppermute(y, "rows", [(i, i ^ reach) for i in range(n)])

    splits = []
    reach = 1
    while reach < n:
        half = x.shape[0] // 2
        if len(splits) < 3 and half % BLOCK == 0:
            bit = lax.rem(lax.div(me, reach), 2)
            kept = lax.dynamic_slice_in_dim(x, bit * half, half)
            given = lax.dynamic_slice_in_dim(x, (1 - bit) * half, half)
            x = kept + swap(given, reach)
            splits.append((reach, bit))
        else:
            x = x + swap(x, reach)
        reach *= 2
    for reach, bit in reversed(splits):
        other = swap(x, reach)
        x = jnp.where(bit == 0, jnp.concatenate([x, other], 0), jnp.concatenate([other, x], 0))
    return x


def shards(p_left, phi_right, v_cols, w_cols, residual):
    rank, local = p_left.shape
    cols = v_cols.shape[0]
    n = lax.axis_size("rows")
    mine = sort_by_owner(p_left, w_cols, n)
    owned = lax.all_to_all(mine, "rows", split_axis=0, concat_axis=0, tiled=True)
    packed = sum_over_rows(packed_grams(p_left, w_cols, phi_right, v_cols, residual))
    k_left, k_right, u, rms = small_algebra(packed, rank, cols, float(local * n))
    update, q_right = right_products(p_left, w_cols, phi_right, v_cols, k_right, u)
    q_left = left_products(owned, k_left)
    return (update.reshape(local), q_left, q_right, rms[0, 0:2])


def solution(mesh):
    placed = (P(None, "rows"), P(None, "rows"), P(None, "rows"), P(None, "rows"), P("rows"))
    return jax.shard_map(
        shards,
        mesh=mesh,
        in_specs=placed,
        out_specs=(P("rows"), P(None, "rows"), P(None, "rows"), P()),
        check_vma=False,
    )
```

```python
import functools

import jax
import jax.numpy as jnp
from jax import lax
from jax.experimental import pallas as pl
from jax.experimental.pallas import tpu as pltpu
from jax.sharding import PartitionSpec as P

SINGLE = jnp.float32
HALF = jnp.bfloat16
LANES = 128
BLOCK = 8
HIGHEST = lax.Precision.HIGHEST
NT = (((1,), (1,)), ((), ()))
VMEM_LIMIT = 24 * 1024 * 1024
SORT_TILE = 256


def iota(shape, dim):
    return lax.broadcasted_iota(jnp.int32, shape, dim)


def dot_hi(a, b, dims=None):
    if dims is None:
        return jnp.dot(a, b, precision=HIGHEST, preferred_element_type=SINGLE)
    return lax.dot_general(a, b, dims, precision=HIGHEST, preferred_element_type=SINGLE)


def in_vmem(x):
    return pltpu.with_memory_space_constraint(x, pltpu.VMEM)


def in_hbm(*xs):
    return [pltpu.with_memory_space_constraint(x, pltpu.HBM) for x in xs]


def to_half(x):
    return x.astype(HALF).astype(SINGLE)


def sort_kernel(n, p_ref, w_ref, out_ref, turned):
    cross = out_ref.shape[1]
    wide = p_ref.shape[1]
    tile = SORT_TILE
    runs = tile // n
    row, column = iota((tile, tile), 0), iota((tile, tile), 1)
    wanted = lax.rem(row, runs) * n + lax.div(row, runs)
    permutation = jnp.where(column == wanted, 1.0, 0.0).astype(HALF)
    eye = jnp.where(iota((cross, cross), 0) == iota((cross, cross), 1), 1.0, 0.0).astype(HALF)
    pair = 16 // runs if runs < 16 else 1
    for at in range(0, wide, tile * pair):
        parts = []
        for i in range(pair):
            cut = slice(at + i * tile, at + (i + 1) * tile)
            both = jnp.concatenate([p_ref[:, cut].astype(SINGLE), w_ref[:, cut].astype(SINGLE)], 0)
            part = lax.dot_general(permutation, both.astype(HALF), NT, preferred_element_type=SINGLE)
            parts.append(part.reshape(n, runs, cross))
        rows = slice(at // n, at // n + runs * pair)
        turned[:, rows, :] = jnp.concatenate(parts, 1).astype(HALF)
    for owner in range(n):
        mine = lax.dot_general(eye, turned[owner], NT, preferred_element_type=SINGLE)
        out_ref[owner] = mine.astype(HALF)


def sort_by_owner(p_left, w_cols, n):
    rank, local = p_left.shape
    cols = w_cols.shape[0]
    share = local // n
    chunks = share // LANES if share % LANES == 0 else 1
    wide = local // chunks
    return pl.pallas_call(
        functools.partial(sort_kernel, n),
        grid=(chunks,),
        in_specs=[
            pl.BlockSpec((rank, wide), lambda i: (0, i)),
            pl.BlockSpec((cols, wide), lambda i: (0, i)),
        ],
        out_specs=pl.BlockSpec((n, rank + cols, share // chunks), lambda i: (0, 0, i)),
        out_shape=pltpu.HBM((n, rank + cols, share), HALF),
        scratch_shapes=[pltpu.VMEM((n, share // chunks, rank + cols), HALF)],
        compiler_params=pltpu.CompilerParams(vmem_limit_bytes=VMEM_LIMIT),
        name="sort_by_owner",
    )(*in_hbm(p_left, w_cols))


def gram_kernel(p_ref, w_ref, phi_ref, v_ref, res_ref, out_ref, left, right):
    at = pl.program_id(0)

    @pl.when(at == 0)
    def _():
        left[...] = jnp.zeros_like(left)
        right[...] = jnp.zeros_like(right)

    x = jnp.concatenate([p_ref[...].astype(SINGLE), w_ref[...].astype(SINGLE)], 0).astype(HALF)
    left[...] += lax.dot_general(x, x, NT, preferred_element_type=SINGLE)
    wide = res_ref.shape[1]
    last = jnp.where(iota((8, wide), 0) == 0, res_ref[...].astype(SINGLE), 0.0)
    y = jnp.concatenate([phi_ref[...].astype(SINGLE), v_ref[...].astype(SINGLE), last], 0).astype(HALF)
    right[...] += lax.dot_general(y, y, NT, preferred_element_type=SINGLE)

    @pl.when(at == pl.num_programs(0) - 1)
    def _():
        cross = left.shape[0]
        m = LANES
        e = cross - m
        rows, lanes = iota((m, m), 0), iota((m, m), 1)
        top_right = right[0:m, 0:m]
        out_ref[0:m, :] = jnp.where(lanes <= rows, left[0:m, 0:m], top_right)
        out_ref[m : m + e, :] = left[m:cross, 0:m]
        out_ref[m + e : m + 2 * e, :] = right[m:cross, 0:m]
        out_ref[m + 2 * e : m + 3 * e, :] = jnp.zeros((e, m), SINGLE)
        out_ref[m + 2 * e : m + 3 * e, 0:e] = left[m:cross, m:cross]
        out_ref[m + 2 * e : m + 3 * e, e : 2 * e] = right[m:cross, m:cross]
        base = m + 3 * e
        out_ref[base:, :] = jnp.zeros((out_ref.shape[0] - base, m), SINGLE)
        out_ref[base : base + 1, :] = jnp.sum(jnp.where(rows == lanes, top_right, 0.0), 0, keepdims=True)
        out_ref[base + 1 : base + 2, :] = right[cross : cross + 1, 0:m]
        out_ref[base + 2 : base + 3, 0 : e + 1] = right[cross : cross + 1, m : cross + 1]


def packed_rows(cross):
    used = LANES + 3 * (cross - LANES) + BLOCK
    return -(-used // (8 * BLOCK)) * 8 * BLOCK


def packed_grams(p_left, w_cols, phi_right, v_cols, residual):
    rank, local = p_left.shape
    cols = w_cols.shape[0]
    cross = rank + cols
    wide = min(local, 2048)
    spec = lambda rows: pl.BlockSpec((rows, wide), lambda i: (0, i))
    return pl.pallas_call(
        gram_kernel,
        grid=(local // wide,),
        in_specs=[spec(rank), spec(cols), spec(rank), spec(cols), spec(1)],
        out_specs=pl.BlockSpec((packed_rows(cross), LANES), lambda i: (0, 0)),
        out_shape=pltpu.VMEM((packed_rows(cross), LANES), SINGLE),
        scratch_shapes=[pltpu.VMEM((cross, cross), SINGLE), pltpu.VMEM((cross + 8, cross + 8), SINGLE)],
        compiler_params=pltpu.CompilerParams(vmem_limit_bytes=VMEM_LIMIT),
        name="packed_grams",
    )(*in_hbm(p_left, w_cols, phi_right, v_cols), residual.reshape(1, local))


def eliminate(refs, tops, k):
    panels = []
    for ref, top in zip(refs, tops):
        cross = ref.shape[1]
        x = ref[pl.ds(pl.multiple_of(k - top, BLOCK), BLOCK), :]
        lane, sub = iota((BLOCK, cross), 1), iota((BLOCK, cross), 0)
        column = [
            jnp.sum(jnp.where(lane == k + i, x, 0.0), 1, keepdims=True) for i in range(BLOCK)
        ]
        rel = lane - k
        x = jnp.where((rel >= 0) & (rel < BLOCK), jnp.where(rel == sub, 1.0, 0.0), x)
        panels.append([x, column, rel, sub])
    thin = iota((BLOCK, 1), 0)
    for i in range(BLOCK):
        for panel in panels:
            x, column, rel, sub = panel
            scale = lax.rsqrt(column[i][i : i + 1, :])
            factor = jnp.where(thin > i, column[i] * scale, 0.0)
            for j in range(i + 1, BLOCK):
                column[j] = column[j] - factor * (column[j][i : i + 1, :] * scale)
            row = x[i : i + 1, :] * scale
            panel[0] = jnp.where(sub == i, row, x - factor * row)
    for ref, top, (x, _, rel, _) in zip(refs, tops, panels):
        cross = ref.shape[1]
        right = jnp.where(rel >= BLOCK, x, 0.0)
        done = jnp.where(rel < BLOCK, x, 0.0)
        r0 = to_half(right)
        r1 = to_half(right - r0)
        r2 = right - r0 - r1
        x0 = to_half(x)
        x1 = to_half(x - x0)
        x2 = x - x0 - x1
        lhs = jnp.concatenate([r0, r0, r0, r1, r1, r2], 0)
        if top:
            lhs = jnp.concatenate([lhs, jnp.zeros((LANES - lhs.shape[0], cross), SINGLE)], 0)
            lhs = lhs.T[top:cross, 0 : 6 * BLOCK].astype(HALF)
        else:
            lhs = lhs.T.astype(HALF)
        rhs = jnp.concatenate([x0, x1, x2, x0, x1, x0], 0).astype(HALF)
        change = jnp.dot(lhs, rhs, preferred_element_type=SINGLE)
        here = iota(ref.shape, 1) - k
        ref[...] = jnp.where((here >= 0) & (here < BLOCK), 0.0, ref[...]) - change
        ref[pl.ds(pl.multiple_of(k - top, BLOCK), BLOCK), :] = done


def small_kernel(rank, count, g_ref, kl_ref, kr_ref, u_ref, rms_ref, left, right, tail):
    cross = left.shape[0]
    m = LANES
    e = cross - m
    base = m + 3 * e
    rows, lanes = iota((m, m), 0), iota((m, m), 1)
    top = g_ref[0:m, :]
    lower = jnp.where(lanes < rows, top, 0.0)
    upper = jnp.where(lanes > rows, top, 0.0)
    same = rows == lanes
    left[0:m, 0:m] = lower + lower.T + jnp.where(same, top, 0.0)
    right[0:m, 0:m] = upper + upper.T + jnp.where(same, g_ref[base : base + 1, :], 0.0)
    left[m:cross, 0:m] = g_ref[m : m + e, :]
    right[m:cross, 0:m] = g_ref[m + e : m + 2 * e, :]
    left[0:m, m:cross] = g_ref[m : m + e, :].T
    right[0:m, m:cross] = g_ref[m + e : m + 2 * e, :].T
    left[m:cross, m:cross] = g_ref[m + 2 * e : m + 3 * e, 0:e]
    right[m:cross, m:cross] = g_ref[m + 2 * e : m + 3 * e, e : 2 * e]
    g_left = left[...]
    g_right = right[...]
    res_first = g_ref[base + 1 : base + 2, :]
    res_rest = g_ref[base + 2 : base + 3, 0:e]
    res_row = jnp.concatenate([res_first, res_rest], 1)
    res_sq = g_ref[base + 2 : base + 3, e : e + 1]

    tail[...] = g_right[rank:cross, :]
    lax.fori_loop(
        rank // BLOCK, cross // BLOCK, lambda b, c: (eliminate([tail], [rank], b * BLOCK), c)[1], 0
    )
    low_lane = iota((cross - rank, cross), 1)
    low_row = iota((cross - rank, cross), 0)
    inverse = jnp.where(low_lane >= rank, tail[...], 0.0)
    eye = jnp.where(iota((rank, cross), 0) == iota((rank, cross), 1), 1.0, 0.0)

    mix = jnp.where(
        low_lane < rank, -to_half(g_right[rank:cross, :]), jnp.where(low_lane == low_row + rank, 1.0, 0.0)
    )
    to_tilde = jnp.concatenate([eye, mix], 0)
    t_right = jnp.concatenate([eye, inverse], 0)
    t_left = jnp.concatenate([eye, dot_hi(inverse, to_tilde)], 0)

    lane8 = iota((BLOCK, cross), 1)
    res8 = jnp.broadcast_to(res_row, (BLOCK, cross))
    half_way = dot_hi(jnp.where(lane8 >= rank, res8, 0.0), inverse, NT)
    coeffs = -dot_hi(half_way, inverse)
    u = dot_hi(jnp.where(lane8 < rank, -to_half(res8), coeffs), to_tilde)
    upd_sq = jnp.sum(dot_hi(u, g_left) * u, 1, keepdims=True)[0:1, :]
    u0 = to_half(u)
    u1 = to_half(u - u0)
    u2 = u - u0 - u1
    sub8 = iota((BLOCK, cross), 0)
    u_ref[...] = jnp.where(sub8 == 0, u0, jnp.where(sub8 == 1, u1, jnp.where(sub8 == 2, u2, 0.0)))
    lane_out = iota((1, LANES), 1)
    rms_ref[...] = jnp.sqrt(jnp.where(lane_out == 0, res_sq, upd_sq) / count)

    left[...] = dot_hi(dot_hi(t_left, g_left), t_left, NT)
    right[...] = dot_hi(dot_hi(t_right, g_right), t_right, NT)
    lax.fori_loop(
        0, cross // BLOCK, lambda b, c: (eliminate([left, right], [0, 0], b * BLOCK), c)[1], 0
    )
    for source, turn, out in ((left, t_left, kl_ref), (right, t_right, kr_ref)):
        k = dot_hi(source[...], turn)
        k0 = to_half(k)
        out[0:cross, :] = k0.astype(HALF)
        out[cross : 2 * cross, :] = (k - k0).astype(HALF)


def small_algebra(packed, rank, cols, count):
    cross = rank + cols
    vmem = pl.BlockSpec(memory_space=pltpu.VMEM)
    return pl.pallas_call(
        functools.partial(small_kernel, rank, count),
        in_specs=[vmem],
        out_specs=[vmem] * 4,
        out_shape=[
            pltpu.VMEM((2 * cross, cross), HALF),
            pltpu.VMEM((2 * cross, cross), HALF),
            pltpu.VMEM((BLOCK, cross), SINGLE),
            jax.ShapeDtypeStruct((1, LANES), SINGLE),
        ],
        scratch_shapes=[
            pltpu.VMEM((cross, cross), SINGLE),
            pltpu.VMEM((cross, cross), SINGLE),
            pltpu.VMEM((cols, cross), SINGLE),
        ],
        compiler_params=pltpu.CompilerParams(vmem_limit_bytes=VMEM_LIMIT),
        name="small_algebra",
    )(in_vmem(packed))


def right_kernel(p_ref, w_ref, phi_ref, v_ref, k_ref, u_ref, upd_ref, q_ref):
    cross = k_ref.shape[1]
    y = jnp.concatenate([phi_ref[...].astype(SINGLE), v_ref[...].astype(SINGLE)], 0).astype(HALF)
    both = jnp.dot(k_ref[...], y, preferred_element_type=SINGLE)
    q_ref[...] = (both[0:cross] + both[cross : 2 * cross]).astype(HALF)
    x = jnp.concatenate([p_ref[...].astype(SINGLE), w_ref[...].astype(SINGLE)], 0).astype(HALF)
    upd_ref[...] = jnp.sum(
        jnp.dot(u_ref[...].astype(HALF), x, preferred_element_type=SINGLE), 0, keepdims=True
    )


def right_products(p_left, w_cols, phi_right, v_cols, k_right, u):
    rank, local = p_left.shape
    cols = w_cols.shape[0]
    cross = rank + cols
    wide = min(local, 2048)
    spec = lambda rows: pl.BlockSpec((rows, wide), lambda i: (0, i))
    return pl.pallas_call(
        right_kernel,
        grid=(local // wide,),
        in_specs=[
            spec(rank), spec(cols), spec(rank), spec(cols),
            pl.BlockSpec((2 * cross, cross), lambda i: (0, 0)),
            pl.BlockSpec((BLOCK, cross), lambda i: (0, 0)),
        ],
        out_specs=[spec(1), spec(cross)],
        out_shape=[
            jax.ShapeDtypeStruct((1, local), SINGLE),
            jax.ShapeDtypeStruct((cross, local), HALF),
        ],
        compiler_params=pltpu.CompilerParams(vmem_limit_bytes=VMEM_LIMIT),
        name="right_products",
    )(*in_hbm(p_left, w_cols, phi_right, v_cols), in_vmem(k_right), in_vmem(u))


def left_kernel(x_ref, k_ref, q_ref):
    group, cross, share = x_ref.shape
    for i in range(group):
        both = jnp.dot(k_ref[...], x_ref[i], preferred_element_type=SINGLE)
        q_ref[:, i * share : (i + 1) * share] = (both[0:cross] + both[cross : 2 * cross]).astype(HALF)


def left_products(sorted_x, k_left):
    n, cross, share = sorted_x.shape
    group = max(1, 2048 // share)
    return pl.pallas_call(
        left_kernel,
        grid=(n // group,),
        in_specs=[
            pl.BlockSpec((group, cross, share), lambda i: (i, 0, 0)),
            pl.BlockSpec((2 * cross, cross), lambda i: (0, 0)),
        ],
        out_specs=pl.BlockSpec((cross, group * share), lambda i: (0, i)),
        out_shape=jax.ShapeDtypeStruct((cross, n * share), HALF),
        compiler_params=pltpu.CompilerParams(vmem_limit_bytes=VMEM_LIMIT),
        name="left_products",
    )(in_vmem(sorted_x), in_vmem(k_left))


def swap(x, reach):
    n = lax.axis_size("rows")
    return lax.ppermute(x, "rows", [(i, i ^ reach) for i in range(n)])


def sum_over_rest(x, reaches):
    me = lax.axis_index("rows")
    splits = []
    for reach in reaches:
        half = x.shape[0] // 2
        bit = lax.rem(lax.div(me, reach), 2)
        kept = lax.dynamic_slice_in_dim(x, bit * half, half)
        given = lax.dynamic_slice_in_dim(x, (1 - bit) * half, half)
        x = kept + swap(given, reach)
        splits.append((reach, bit))
    for reach, bit in reversed(splits):
        other = swap(x, reach)
        x = jnp.where(bit == 0, jnp.concatenate([x, other], 0), jnp.concatenate([other, x], 0))
    return x


def shards(p_left, phi_right, v_cols, w_cols, residual):
    rank, local = p_left.shape
    cols = v_cols.shape[0]
    n = lax.axis_size("rows")
    near = [1 << i for i in range(3)]
    far = [1 << i for i in range(3, n.bit_length() - 1)]
    packed = packed_grams(p_left, w_cols, phi_right, v_cols, residual)
    mine = sort_by_owner(p_left, w_cols, n)
    for reach in far[:-1]:
        packed = packed + swap(packed, reach)
    mine, packed = lax.optimization_barrier((mine, packed))
    other = swap(packed, far[-1])
    owned = lax.all_to_all(mine, "rows", split_axis=0, concat_axis=0, tiled=True)
    packed = packed + other
    packed = sum_over_rest(packed, near)
    k_left, k_right, u, rms = small_algebra(packed, rank, cols, float(local * n))
    update, q_right = right_products(p_left, w_cols, phi_right, v_cols, k_right, u)
    q_left = left_products(owned, k_left)
    return (update.reshape(local), q_left, q_right, rms[0, 0:2])


def solution(mesh):
    placed = (P(None, "rows"), P(None, "rows"), P(None, "rows"), P(None, "rows"), P("rows"))
    return jax.shard_map(
        shards,
        mesh=mesh,
        in_specs=placed,
        out_specs=(P("rows"), P(None, "rows"), P(None, "rows"), P()),
        check_vma=False,
    )
```

```python
import functools

import jax
import jax.numpy as jnp
from jax import lax
from jax.experimental import pallas as pl
from jax.experimental.pallas import tpu as pltpu
from jax.sharding import PartitionSpec as P

SINGLE = jnp.float32
HALF = jnp.bfloat16
LANES = 128
BLOCK = 8
HIGHEST = lax.Precision.HIGHEST
NT = (((1,), (1,)), ((), ()))
VMEM_LIMIT = 24 * 1024 * 1024
SORT_TILE = 256


def iota(shape, dim):
    return lax.broadcasted_iota(jnp.int32, shape, dim)


def dot_hi(a, b, dims=None):
    if dims is None:
        return jnp.dot(a, b, precision=HIGHEST, preferred_element_type=SINGLE)
    return lax.dot_general(a, b, dims, precision=HIGHEST, preferred_element_type=SINGLE)


def in_vmem(x):
    return pltpu.with_memory_space_constraint(x, pltpu.VMEM)


def in_hbm(*xs):
    return [pltpu.with_memory_space_constraint(x, pltpu.HBM) for x in xs]


def to_half(x):
    return x.astype(HALF).astype(SINGLE)


def sort_kernel(n, x_ref, out_ref, turned, ready, sem):
    cross, local = x_ref.shape
    tile = SORT_TILE
    runs = tile // n
    row, column = iota((tile, tile), 0), iota((tile, tile), 1)
    wanted = lax.rem(row, runs) * n + lax.div(row, runs)
    permutation = jnp.where(column == wanted, 1.0, 0.0).astype(HALF)
    eye = jnp.where(iota((cross, cross), 0) == iota((cross, cross), 1), 1.0, 0.0).astype(HALF)
    pair = 16 // runs if runs < 16 else 1
    for at in range(0, local, tile * pair):
        parts = []
        for i in range(pair):
            x = x_ref[:, at + i * tile : at + (i + 1) * tile]
            part = lax.dot_general(permutation, x, NT, preferred_element_type=SINGLE)
            parts.append(part.reshape(n, runs, cross))
        rows = slice(at // n, at // n + runs * pair)
        turned[:, rows, :] = jnp.concatenate(parts, 1).astype(HALF)
    copies = []
    for owner in range(n):
        mine = lax.dot_general(eye, turned[owner], NT, preferred_element_type=SINGLE)
        ready[owner] = mine.astype(HALF)
        copies.append(pltpu.make_async_copy(ready.at[owner], out_ref.at[owner], sem.at[owner]))
        copies[-1].start()
    for copy in copies:
        copy.wait()


def sort_by_owner(x, n):
    cross, local = x.shape
    share = local // n
    return pl.pallas_call(
        functools.partial(sort_kernel, n),
        in_specs=[pl.BlockSpec(memory_space=pltpu.VMEM)],
        out_specs=pl.BlockSpec(memory_space=pltpu.HBM),
        out_shape=pltpu.HBM((n, cross, share), HALF),
        scratch_shapes=[
            pltpu.VMEM((n, share, cross), HALF),
            pltpu.VMEM((n, cross, share), HALF),
            pltpu.SemaphoreType.DMA((n,)),
        ],
        compiler_params=pltpu.CompilerParams(vmem_limit_bytes=VMEM_LIMIT),
        name="sort_by_owner",
    )(in_vmem(x))


def gram_kernel(chunks, p_hbm, w_hbm, phi_hbm, v_hbm, res_hbm, out_ref, x_ref, *scratch):
    *buffers, left, right, sem = scratch
    sources = (p_hbm, w_hbm, phi_hbm, v_hbm)
    wide = x_ref.shape[1] // chunks
    res_buffer = buffers[-1]
    res_copy = pltpu.make_async_copy(res_hbm, res_buffer, sem.at[len(sources), 0])
    copies = []
    for at in range(chunks):
        cut = pl.ds(at * wide, wide)
        copies.append(
            [
                pltpu.make_async_copy(source.at[:, cut], buffer.at[:, cut], sem.at[i, at])
                for i, (source, buffer) in enumerate(zip(sources, buffers))
            ]
        )
        for copy in copies[-1]:
            copy.start()
        if at == 0:
            res_copy.start()
    for at in range(chunks):
        cut = slice(at * wide, (at + 1) * wide)
        for copy in copies[at]:
            copy.wait()
        if at == 0:
            res_copy.wait()
        p, w, phi, v = [buffer[:, cut].astype(SINGLE) for buffer in buffers[:4]]
        x = jnp.concatenate([p, w], 0).astype(HALF)
        x_ref[:, cut] = x
        more = lax.dot_general(x, x, NT, preferred_element_type=SINGLE)
        left[...] = more if at == 0 else left[...] + more
        y = jnp.concatenate([phi, v], 0).astype(HALF)
        res = res_buffer[cut].astype(SINGLE).reshape(1, wide)
        last = jnp.where(iota((16, wide), 0) == 0, res, 0.0).astype(HALF)
        z = jnp.concatenate([y, last], 0)
        more = lax.dot_general(z, z, NT, preferred_element_type=SINGLE)
        right[...] = more if at == 0 else right[...] + more
    cross = left.shape[0]
    m = LANES
    e = cross - m
    rows, lanes = iota((m, m), 0), iota((m, m), 1)
    top_right = right[0:m, 0:m]
    out_ref[0:m, :] = jnp.where(lanes <= rows, left[0:m, 0:m], top_right)
    out_ref[m : m + e, :] = left[m:cross, 0:m]
    out_ref[m + e : m + 2 * e, :] = right[m:cross, 0:m]
    out_ref[m + 2 * e : m + 3 * e, :] = jnp.zeros((e, m), SINGLE)
    out_ref[m + 2 * e : m + 3 * e, 0:e] = left[m:cross, m:cross]
    out_ref[m + 2 * e : m + 3 * e, e : 2 * e] = right[m:cross, m:cross]
    base = m + 3 * e
    out_ref[base:, :] = jnp.zeros((out_ref.shape[0] - base, m), SINGLE)
    out_ref[base : base + 1, :] = jnp.sum(jnp.where(rows == lanes, top_right, 0.0), 0, keepdims=True)
    out_ref[base + 1 : base + 2, :] = right[cross : cross + 1, 0:m]
    out_ref[base + 2 : base + 3, 0 : e + 1] = right[cross : cross + 1, m : cross + 1]


def packed_rows(cross):
    used = LANES + 3 * (cross - LANES) + BLOCK
    return -(-used // (8 * BLOCK)) * 8 * BLOCK


def packed_grams(p_left, w_cols, phi_right, v_cols, residual):
    rank, local = p_left.shape
    cols = w_cols.shape[0]
    cross = rank + cols
    chunks = 4
    hbm = pl.BlockSpec(memory_space=pltpu.HBM)
    vmem = pl.BlockSpec(memory_space=pltpu.VMEM)
    return pl.pallas_call(
        functools.partial(gram_kernel, chunks),
        in_specs=[hbm] * 5,
        out_specs=[vmem] * 2,
        out_shape=[
            pltpu.VMEM((packed_rows(cross), LANES), SINGLE),
            pltpu.VMEM((cross, local), HALF),
        ],
        scratch_shapes=[
            pltpu.VMEM((rank, local), HALF),
            pltpu.VMEM((cols, local), HALF),
            pltpu.VMEM((rank, local), HALF),
            pltpu.VMEM((cols, local), HALF),
            pltpu.VMEM((local,), HALF),
            pltpu.VMEM((cross, cross), SINGLE),
            pltpu.VMEM((cross + 16, cross + 16), SINGLE),
            pltpu.SemaphoreType.DMA((5, chunks)),
        ],
        compiler_params=pltpu.CompilerParams(vmem_limit_bytes=VMEM_LIMIT),
        name="packed_grams",
    )(*in_hbm(p_left, w_cols, phi_right, v_cols, residual))


def eliminate(refs, tops, k):
    panels = []
    for ref, top in zip(refs, tops):
        cross = ref.shape[1]
        x = ref[pl.ds(pl.multiple_of(k - top, BLOCK), BLOCK), :]
        lane, sub = iota((BLOCK, cross), 1), iota((BLOCK, cross), 0)
        column = [
            jnp.sum(jnp.where(lane == k + i, x, 0.0), 1, keepdims=True) for i in range(BLOCK)
        ]
        rel = lane - k
        x = jnp.where((rel >= 0) & (rel < BLOCK), jnp.where(rel == sub, 1.0, 0.0), x)
        panels.append([x, column, rel, sub])
    thin = iota((BLOCK, 1), 0)
    for i in range(BLOCK):
        for panel in panels:
            x, column, rel, sub = panel
            scale = lax.rsqrt(column[i][i : i + 1, :])
            factor = jnp.where(thin > i, column[i] * scale, 0.0)
            for j in range(i + 1, BLOCK):
                column[j] = column[j] - factor * (column[j][i : i + 1, :] * scale)
            row = x[i : i + 1, :] * scale
            panel[0] = jnp.where(sub == i, row, x - factor * row)
    for ref, top, (x, _, rel, _) in zip(refs, tops, panels):
        cross = ref.shape[1]
        right = jnp.where(rel >= BLOCK, x, 0.0)
        done = jnp.where(rel < BLOCK, x, 0.0)
        r0 = to_half(right)
        r1 = to_half(right - r0)
        r2 = right - r0 - r1
        x0 = to_half(x)
        x1 = to_half(x - x0)
        x2 = x - x0 - x1
        lhs = jnp.concatenate([r0, r0, r0, r1, r1, r2], 0)
        if top:
            lhs = jnp.concatenate([lhs, jnp.zeros((LANES - lhs.shape[0], cross), SINGLE)], 0)
            lhs = lhs.T[top:cross, 0 : 6 * BLOCK].astype(HALF)
        else:
            lhs = lhs.T.astype(HALF)
        rhs = jnp.concatenate([x0, x1, x2, x0, x1, x0], 0).astype(HALF)
        change = jnp.dot(lhs, rhs, preferred_element_type=SINGLE)
        here = iota(ref.shape, 1) - k
        ref[...] = jnp.where((here >= 0) & (here < BLOCK), 0.0, ref[...]) - change
        ref[pl.ds(pl.multiple_of(k - top, BLOCK), BLOCK), :] = done


def small_kernel(rank, count, g_ref, kl_ref, kr_ref, u_ref, rms_ref, left, right, tail):
    cross = left.shape[0]
    m = LANES
    e = cross - m
    base = m + 3 * e
    rows, lanes = iota((m, m), 0), iota((m, m), 1)
    top = g_ref[0:m, :]
    lower = jnp.where(lanes < rows, top, 0.0)
    upper = jnp.where(lanes > rows, top, 0.0)
    same = rows == lanes
    left[0:m, 0:m] = lower + lower.T + jnp.where(same, top, 0.0)
    right[0:m, 0:m] = upper + upper.T + jnp.where(same, g_ref[base : base + 1, :], 0.0)
    left[m:cross, 0:m] = g_ref[m : m + e, :]
    right[m:cross, 0:m] = g_ref[m + e : m + 2 * e, :]
    left[0:m, m:cross] = g_ref[m : m + e, :].T
    right[0:m, m:cross] = g_ref[m + e : m + 2 * e, :].T
    left[m:cross, m:cross] = g_ref[m + 2 * e : m + 3 * e, 0:e]
    right[m:cross, m:cross] = g_ref[m + 2 * e : m + 3 * e, e : 2 * e]
    g_left = left[...]
    g_right = right[...]
    res_first = g_ref[base + 1 : base + 2, :]
    res_rest = g_ref[base + 2 : base + 3, 0:e]
    res_row = jnp.concatenate([res_first, res_rest], 1)
    res_sq = g_ref[base + 2 : base + 3, e : e + 1]

    tail[...] = g_right[rank:cross, :]
    lax.fori_loop(
        rank // BLOCK, cross // BLOCK, lambda b, c: (eliminate([tail], [rank], b * BLOCK), c)[1], 0
    )
    low_lane = iota((cross - rank, cross), 1)
    low_row = iota((cross - rank, cross), 0)
    inverse = jnp.where(low_lane >= rank, tail[...], 0.0)
    eye = jnp.where(iota((rank, cross), 0) == iota((rank, cross), 1), 1.0, 0.0)

    mix = jnp.where(
        low_lane < rank, -to_half(g_right[rank:cross, :]), jnp.where(low_lane == low_row + rank, 1.0, 0.0)
    )
    to_tilde = jnp.concatenate([eye, mix], 0)
    t_right = jnp.concatenate([eye, inverse], 0)
    t_left = jnp.concatenate([eye, dot_hi(inverse, to_tilde)], 0)

    lane8 = iota((BLOCK, cross), 1)
    res8 = jnp.broadcast_to(res_row, (BLOCK, cross))
    half_way = dot_hi(jnp.where(lane8 >= rank, res8, 0.0), inverse, NT)
    coeffs = -dot_hi(half_way, inverse)
    u = dot_hi(jnp.where(lane8 < rank, -to_half(res8), coeffs), to_tilde)
    upd_sq = jnp.sum(dot_hi(u, g_left) * u, 1, keepdims=True)[0:1, :]
    u0 = to_half(u)
    u1 = to_half(u - u0)
    u2 = u - u0 - u1
    sub8 = iota((BLOCK, cross), 0)
    u_ref[...] = jnp.where(sub8 == 0, u0, jnp.where(sub8 == 1, u1, jnp.where(sub8 == 2, u2, 0.0)))
    lane_out = iota((1, LANES), 1)
    rms_ref[...] = jnp.sqrt(jnp.where(lane_out == 0, res_sq, upd_sq) / count)

    left[...] = dot_hi(dot_hi(t_left, g_left), t_left, NT)
    right[...] = dot_hi(dot_hi(t_right, g_right), t_right, NT)
    lax.fori_loop(
        0, cross // BLOCK, lambda b, c: (eliminate([left, right], [0, 0], b * BLOCK), c)[1], 0
    )
    for source, turn, out in ((left, t_left, kl_ref), (right, t_right, kr_ref)):
        k = dot_hi(source[...], turn)
        k0 = to_half(k)
        out[0:cross, :] = k0.astype(HALF)
        out[cross : 2 * cross, :] = (k - k0).astype(HALF)


def small_algebra(packed, rank, cols, count):
    cross = rank + cols
    vmem = pl.BlockSpec(memory_space=pltpu.VMEM)
    return pl.pallas_call(
        functools.partial(small_kernel, rank, count),
        in_specs=[vmem],
        out_specs=[vmem] * 4,
        out_shape=[
            pltpu.VMEM((2 * cross, cross), HALF),
            pltpu.VMEM((2 * cross, cross), HALF),
            pltpu.VMEM((BLOCK, cross), SINGLE),
            jax.ShapeDtypeStruct((1, LANES), SINGLE),
        ],
        scratch_shapes=[
            pltpu.VMEM((cross, cross), SINGLE),
            pltpu.VMEM((cross, cross), SINGLE),
            pltpu.VMEM((cols, cross), SINGLE),
        ],
        compiler_params=pltpu.CompilerParams(vmem_limit_bytes=VMEM_LIMIT),
        name="small_algebra",
    )(in_vmem(packed))


def right_kernel(p_ref, w_ref, phi_ref, v_ref, k_ref, u_ref, upd_ref, q_ref):
    cross = k_ref.shape[1]
    y = jnp.concatenate([phi_ref[...].astype(SINGLE), v_ref[...].astype(SINGLE)], 0).astype(HALF)
    both = jnp.dot(k_ref[...], y, preferred_element_type=SINGLE)
    q_ref[...] = (both[0:cross] + both[cross : 2 * cross]).astype(HALF)
    x = jnp.concatenate([p_ref[...].astype(SINGLE), w_ref[...].astype(SINGLE)], 0).astype(HALF)
    upd_ref[...] = jnp.sum(
        jnp.dot(u_ref[...].astype(HALF), x, preferred_element_type=SINGLE), 0, keepdims=True
    )


def right_products(p_left, w_cols, phi_right, v_cols, k_right, u):
    rank, local = p_left.shape
    cols = w_cols.shape[0]
    cross = rank + cols
    wide = min(local, 2048)
    spec = lambda rows: pl.BlockSpec((rows, wide), lambda i: (0, i))
    return pl.pallas_call(
        right_kernel,
        grid=(local // wide,),
        in_specs=[
            spec(rank), spec(cols), spec(rank), spec(cols),
            pl.BlockSpec((2 * cross, cross), lambda i: (0, 0)),
            pl.BlockSpec((BLOCK, cross), lambda i: (0, 0)),
        ],
        out_specs=[spec(1), spec(cross)],
        out_shape=[
            jax.ShapeDtypeStruct((1, local), SINGLE),
            pltpu.HBM((cross, local), HALF),
        ],
        compiler_params=pltpu.CompilerParams(vmem_limit_bytes=VMEM_LIMIT),
        name="right_products",
    )(*in_hbm(p_left, w_cols, phi_right, v_cols), in_vmem(k_right), in_vmem(u))


def left_kernel(x_ref, k_ref, q_ref):
    group, cross, share = x_ref.shape
    for i in range(group):
        both = jnp.dot(k_ref[...], x_ref[i], preferred_element_type=SINGLE)
        q_ref[:, i * share : (i + 1) * share] = (both[0:cross] + both[cross : 2 * cross]).astype(HALF)


def left_products(sorted_x, k_left):
    n, cross, share = sorted_x.shape
    group = max(1, 2048 // share)
    return pl.pallas_call(
        left_kernel,
        grid=(n // group,),
        in_specs=[
            pl.BlockSpec((group, cross, share), lambda i: (i, 0, 0)),
            pl.BlockSpec((2 * cross, cross), lambda i: (0, 0)),
        ],
        out_specs=pl.BlockSpec((cross, group * share), lambda i: (0, i)),
        out_shape=jax.ShapeDtypeStruct((cross, n * share), HALF),
        compiler_params=pltpu.CompilerParams(vmem_limit_bytes=VMEM_LIMIT),
        name="left_products",
    )(in_vmem(sorted_x), in_vmem(k_left))


def swap(x, reach):
    n = lax.axis_size("rows")
    return lax.ppermute(x, "rows", [(i, i ^ reach) for i in range(n)])


def split(x, reach):
    half = x.shape[0] // 2
    bit = lax.rem(lax.div(lax.axis_index("rows"), reach), 2)
    kept = lax.dynamic_slice_in_dim(x, bit * half, half)
    given = lax.dynamic_slice_in_dim(x, (1 - bit) * half, half)
    return kept + swap(given, reach)


def join(x, reach):
    bit = lax.rem(lax.div(lax.axis_index("rows"), reach), 2)
    other = swap(x, reach)
    return jnp.where(bit == 0, jnp.concatenate([x, other], 0), jnp.concatenate([other, x], 0))


def shards(p_left, phi_right, v_cols, w_cols, residual):
    rank, local = p_left.shape
    cols = v_cols.shape[0]
    n = lax.axis_size("rows")
    near = [1 << i for i in range(3)]
    far = [1 << i for i in range(3, n.bit_length() - 1)]
    packed, x = packed_grams(p_left, w_cols, phi_right, v_cols, residual)
    packed = split(packed, near[0])
    mine = sort_by_owner(x, n)
    for reach in far[:-1]:
        packed = packed + swap(packed, reach)
    mine, packed = lax.optimization_barrier((mine, packed))
    other = swap(packed, far[-1])
    owned = lax.all_to_all(mine, "rows", split_axis=0, concat_axis=0, tiled=True)
    packed = packed + other
    for reach in near[1:]:
        packed = split(packed, reach)
    for reach in reversed(near):
        packed = join(packed, reach)
    k_left, k_right, u, rms = small_algebra(packed, rank, cols, float(local * n))
    update, q_right = right_products(p_left, w_cols, phi_right, v_cols, k_right, u)
    q_left = left_products(owned, k_left)
    return (update.reshape(local), q_left, q_right, rms[0, 0:2])


def solution(mesh):
    placed = (P(None, "rows"), P(None, "rows"), P(None, "rows"), P(None, "rows"), P("rows"))
    return jax.shard_map(
        shards,
        mesh=mesh,
        in_specs=placed,
        out_specs=(P("rows"), P(None, "rows"), P(None, "rows"), P()),
        check_vma=False,
    )
```

```python
import functools

import jax
import jax.numpy as jnp
from jax import lax
from jax.experimental import pallas as pl
from jax.experimental.pallas import tpu as pltpu
from jax.sharding import PartitionSpec as P

SINGLE = jnp.float32
HALF = jnp.bfloat16
LANES = 128
BLOCK = 8
HIGHEST = lax.Precision.HIGHEST
NT = (((1,), (1,)), ((), ()))
VMEM_LIMIT = 24 * 1024 * 1024
SORT_TILE = 256


def iota(shape, dim):
    return lax.broadcasted_iota(jnp.int32, shape, dim)


def dot_hi(a, b, dims=None):
    if dims is None:
        return jnp.dot(a, b, precision=HIGHEST, preferred_element_type=SINGLE)
    return lax.dot_general(a, b, dims, precision=HIGHEST, preferred_element_type=SINGLE)


def in_vmem(x):
    return pltpu.with_memory_space_constraint(x, pltpu.VMEM)


def in_hbm(*xs):
    return [pltpu.with_memory_space_constraint(x, pltpu.HBM) for x in xs]


def to_half(x):
    return x.astype(HALF).astype(SINGLE)


def sort_kernel(n, x_ref, out_ref, turned, ready, sem):
    cross, local = x_ref.shape
    tile = SORT_TILE
    runs = tile // n
    row, column = iota((tile, tile), 0), iota((tile, tile), 1)
    wanted = lax.rem(row, runs) * n + lax.div(row, runs)
    permutation = jnp.where(column == wanted, 1.0, 0.0).astype(HALF)
    eye = jnp.where(iota((cross, cross), 0) == iota((cross, cross), 1), 1.0, 0.0).astype(HALF)
    pair = 16 // runs if runs < 16 else 1
    for at in range(0, local, tile * pair):
        parts = []
        for i in range(pair):
            x = x_ref[:, at + i * tile : at + (i + 1) * tile]
            part = lax.dot_general(permutation, x, NT, preferred_element_type=SINGLE)
            parts.append(part.reshape(n, runs, cross))
        rows = slice(at // n, at // n + runs * pair)
        turned[:, rows, :] = jnp.concatenate(parts, 1).astype(HALF)
    copies = []
    for owner in range(n):
        mine = lax.dot_general(eye, turned[owner], NT, preferred_element_type=SINGLE)
        ready[owner] = mine.astype(HALF)
        copies.append(pltpu.make_async_copy(ready.at[owner], out_ref.at[owner], sem.at[owner]))
        copies[-1].start()
    for copy in copies:
        copy.wait()


def sort_by_owner(x, n):
    cross, local = x.shape
    share = local // n
    return pl.pallas_call(
        functools.partial(sort_kernel, n),
        in_specs=[pl.BlockSpec(memory_space=pltpu.VMEM)],
        out_specs=pl.BlockSpec(memory_space=pltpu.HBM),
        out_shape=pltpu.HBM((n, cross, share), HALF),
        scratch_shapes=[
            pltpu.VMEM((n, share, cross), HALF),
            pltpu.VMEM((n, cross, share), HALF),
            pltpu.SemaphoreType.DMA((n,)),
        ],
        compiler_params=pltpu.CompilerParams(vmem_limit_bytes=VMEM_LIMIT),
        name="sort_by_owner",
    )(in_vmem(x))


def gram_kernel(chunks, p_hbm, w_hbm, phi_hbm, v_hbm, res_hbm, out_ref, x_ref, *scratch):
    *buffers, left, right, sem = scratch
    sources = (p_hbm, w_hbm, phi_hbm, v_hbm)
    wide = x_ref.shape[1] // chunks
    res_buffer = buffers[-1]
    res_copy = pltpu.make_async_copy(res_hbm, res_buffer, sem.at[len(sources), 0])
    copies = []
    for at in range(chunks):
        cut = pl.ds(at * wide, wide)
        copies.append(
            [
                pltpu.make_async_copy(source.at[:, cut], buffer.at[:, cut], sem.at[i, at])
                for i, (source, buffer) in enumerate(zip(sources, buffers))
            ]
        )
        for copy in copies[-1]:
            copy.start()
        if at == 0:
            res_copy.start()
    for at in range(chunks):
        cut = slice(at * wide, (at + 1) * wide)
        for copy in copies[at]:
            copy.wait()
        if at == 0:
            res_copy.wait()
        p, w, phi, v = [buffer[:, cut].astype(SINGLE) for buffer in buffers[:4]]
        x = jnp.concatenate([p, w], 0).astype(HALF)
        x_ref[:, cut] = x
        more = lax.dot_general(x, x, NT, preferred_element_type=SINGLE)
        left[...] = more if at == 0 else left[...] + more
        y = jnp.concatenate([phi, v], 0).astype(HALF)
        res = res_buffer[cut].astype(SINGLE).reshape(1, wide)
        last = jnp.where(iota((16, wide), 0) == 0, res, 0.0).astype(HALF)
        z = jnp.concatenate([y, last], 0)
        more = lax.dot_general(z, z, NT, preferred_element_type=SINGLE)
        right[...] = more if at == 0 else right[...] + more
    cross = left.shape[0]
    m = LANES
    e = cross - m
    top_right = right[0:m, 0:m]
    same = iota((m, m), 0) == iota((m, m), 1)
    out_ref[0:m, :] = jnp.where(iota((m, m), 1) <= iota((m, m), 0), left[0:m, 0:m], top_right)
    out_ref[m : m + e, :] = left[m:cross, 0:m]
    out_ref[m + e : m + 2 * e, :] = right[m:cross, 0:m]
    corner_right = right[m:cross, m:cross]
    lower = iota((e, e), 1) <= iota((e, e), 0)
    corner = jnp.where(lower, left[m:cross, m:cross], corner_right)
    base = m + 2 * e
    out_ref[base : base + 2 * BLOCK, :] = jnp.zeros((2 * BLOCK, m), SINGLE)
    for i in range(e // BLOCK):
        out_ref[base : base + BLOCK, i * e : (i + 1) * e] = corner[i * BLOCK : (i + 1) * BLOCK, :]
    base += BLOCK
    out_ref[base : base + 1, :] = jnp.sum(jnp.where(same, top_right, 0.0), 0, keepdims=True)
    out_ref[base + 1 : base + 2, :] = right[cross : cross + 1, 0:m]
    out_ref[base + 2 : base + 3, 0 : e + 1] = right[cross : cross + 1, m : cross + 1]
    out_ref[base + 3 : base + 4, 0:e] = jnp.sum(
        jnp.where(iota((e, e), 0) == iota((e, e), 1), corner_right, 0.0), 0, keepdims=True
    )


def packed_rows(cross):
    return LANES + 2 * (cross - LANES) + 2 * BLOCK


def packed_grams(p_left, w_cols, phi_right, v_cols, residual):
    rank, local = p_left.shape
    cols = w_cols.shape[0]
    cross = rank + cols
    chunks = 2
    hbm = pl.BlockSpec(memory_space=pltpu.HBM)
    vmem = pl.BlockSpec(memory_space=pltpu.VMEM)
    return pl.pallas_call(
        functools.partial(gram_kernel, chunks),
        in_specs=[hbm] * 5,
        out_specs=[vmem] * 2,
        out_shape=[
            pltpu.VMEM((packed_rows(cross), LANES), SINGLE),
            pltpu.VMEM((cross, local), HALF),
        ],
        scratch_shapes=[
            pltpu.VMEM((rank, local), HALF),
            pltpu.VMEM((cols, local), HALF),
            pltpu.VMEM((rank, local), HALF),
            pltpu.VMEM((cols, local), HALF),
            pltpu.VMEM((local,), HALF),
            pltpu.VMEM((cross, cross), SINGLE),
            pltpu.VMEM((cross + 16, cross + 16), SINGLE),
            pltpu.SemaphoreType.DMA((5, chunks)),
        ],
        compiler_params=pltpu.CompilerParams(vmem_limit_bytes=VMEM_LIMIT),
        name="packed_grams",
    )(*in_hbm(p_left, w_cols, phi_right, v_cols, residual))


def eliminate(refs, tops, k):
    panels = []
    for ref, top in zip(refs, tops):
        cross = ref.shape[1]
        x = ref[pl.ds(pl.multiple_of(k - top, BLOCK), BLOCK), :]
        lane, sub = iota((BLOCK, cross), 1), iota((BLOCK, cross), 0)
        column = [
            jnp.sum(jnp.where(lane == k + i, x, 0.0), 1, keepdims=True) for i in range(BLOCK)
        ]
        rel = lane - k
        x = jnp.where((rel >= 0) & (rel < BLOCK), jnp.where(rel == sub, 1.0, 0.0), x)
        panels.append([x, column, rel, sub])
    thin = iota((BLOCK, 1), 0)
    for i in range(BLOCK):
        for panel in panels:
            x, column, rel, sub = panel
            scale = lax.rsqrt(column[i][i : i + 1, :])
            factor = jnp.where(thin > i, column[i] * scale, 0.0)
            for j in range(i + 1, BLOCK):
                column[j] = column[j] - factor * (column[j][i : i + 1, :] * scale)
            row = x[i : i + 1, :] * scale
            panel[0] = jnp.where(sub == i, row, x - factor * row)
    for ref, top, (x, _, rel, _) in zip(refs, tops, panels):
        cross = ref.shape[1]
        right = jnp.where(rel >= BLOCK, x, 0.0)
        done = jnp.where(rel < BLOCK, x, 0.0)
        r0 = to_half(right)
        r1 = to_half(right - r0)
        r2 = right - r0 - r1
        x0 = to_half(x)
        x1 = to_half(x - x0)
        x2 = x - x0 - x1
        lhs = jnp.concatenate([r0, r0, r0, r1, r1, r2], 0)
        if top:
            lhs = jnp.concatenate([lhs, jnp.zeros((LANES - lhs.shape[0], cross), SINGLE)], 0)
            lhs = lhs.T[top:cross, 0 : 6 * BLOCK].astype(HALF)
        else:
            lhs = lhs.T.astype(HALF)
        rhs = jnp.concatenate([x0, x1, x2, x0, x1, x0], 0).astype(HALF)
        change = jnp.dot(lhs, rhs, preferred_element_type=SINGLE)
        here = iota(ref.shape, 1) - k
        ref[...] = jnp.where((here >= 0) & (here < BLOCK), 0.0, ref[...]) - change
        ref[pl.ds(pl.multiple_of(k - top, BLOCK), BLOCK), :] = done


def small_kernel(rank, count, g_ref, kl_ref, kr_ref, u_ref, rms_ref, left, right, tail):
    cross = left.shape[0]
    m = LANES
    e = cross - m
    base = m + 2 * e + BLOCK

    def unfold(packed, diagonal):
        rows, lanes = iota(packed.shape, 0), iota(packed.shape, 1)
        lower = jnp.where(lanes < rows, packed, 0.0)
        upper = jnp.where(lanes > rows, packed, 0.0)
        same = rows == lanes
        return (
            lower + lower.T + jnp.where(same, packed, 0.0),
            upper + upper.T + jnp.where(same, diagonal, 0.0),
        )

    left[0:m, 0:m], right[0:m, 0:m] = unfold(g_ref[0:m, :], g_ref[base : base + 1, :])
    left[m:cross, 0:m] = g_ref[m : m + e, :]
    right[m:cross, 0:m] = g_ref[m + e : m + 2 * e, :]
    left[0:m, m:cross] = g_ref[m : m + e, :].T
    right[0:m, m:cross] = g_ref[m + e : m + 2 * e, :].T
    corner = jnp.concatenate(
        [g_ref[base - BLOCK : base, i * e : (i + 1) * e] for i in range(e // BLOCK)], 0
    )
    left[m:cross, m:cross], right[m:cross, m:cross] = unfold(corner, g_ref[base + 3 : base + 4, 0:e])
    g_left = left[...]
    g_right = right[...]
    res_first = g_ref[base + 1 : base + 2, :]
    res_rest = g_ref[base + 2 : base + 3, 0:e]
    res_row = jnp.concatenate([res_first, res_rest], 1)
    res_sq = g_ref[base + 2 : base + 3, e : e + 1]

    tail[...] = g_right[rank:cross, :]
    lax.fori_loop(
        rank // BLOCK, cross // BLOCK, lambda b, c: (eliminate([tail], [rank], b * BLOCK), c)[1], 0
    )
    low_lane = iota((cross - rank, cross), 1)
    low_row = iota((cross - rank, cross), 0)
    inverse = jnp.where(low_lane >= rank, tail[...], 0.0)
    eye = jnp.where(iota((rank, cross), 0) == iota((rank, cross), 1), 1.0, 0.0)

    mix = jnp.where(
        low_lane < rank, -to_half(g_right[rank:cross, :]), jnp.where(low_lane == low_row + rank, 1.0, 0.0)
    )
    to_tilde = jnp.concatenate([eye, mix], 0)
    t_right = jnp.concatenate([eye, inverse], 0)
    t_left = jnp.concatenate([eye, dot_hi(inverse, to_tilde)], 0)

    lane8 = iota((BLOCK, cross), 1)
    res8 = jnp.broadcast_to(res_row, (BLOCK, cross))
    half_way = dot_hi(jnp.where(lane8 >= rank, res8, 0.0), inverse, NT)
    coeffs = -dot_hi(half_way, inverse)
    u = dot_hi(jnp.where(lane8 < rank, -to_half(res8), coeffs), to_tilde)
    upd_sq = jnp.sum(dot_hi(u, g_left) * u, 1, keepdims=True)[0:1, :]
    u0 = to_half(u)
    u1 = to_half(u - u0)
    u2 = u - u0 - u1
    sub8 = iota((BLOCK, cross), 0)
    u_ref[...] = jnp.where(sub8 == 0, u0, jnp.where(sub8 == 1, u1, jnp.where(sub8 == 2, u2, 0.0)))
    lane_out = iota((1, LANES), 1)
    rms_ref[...] = jnp.sqrt(jnp.where(lane_out == 0, res_sq, upd_sq) / count)

    left[...] = dot_hi(dot_hi(t_left, g_left), t_left, NT)
    right[...] = dot_hi(dot_hi(t_right, g_right), t_right, NT)
    lax.fori_loop(
        0, cross // BLOCK, lambda b, c: (eliminate([left, right], [0, 0], b * BLOCK), c)[1], 0
    )
    for source, turn, out in ((left, t_left, kl_ref), (right, t_right, kr_ref)):
        k = dot_hi(source[...], turn)
        k0 = to_half(k)
        out[0:cross, :] = k0.astype(HALF)
        out[cross : 2 * cross, :] = (k - k0).astype(HALF)


def small_algebra(packed, rank, cols, count):
    cross = rank + cols
    vmem = pl.BlockSpec(memory_space=pltpu.VMEM)
    return pl.pallas_call(
        functools.partial(small_kernel, rank, count),
        in_specs=[vmem],
        out_specs=[vmem] * 4,
        out_shape=[
            pltpu.VMEM((2 * cross, cross), HALF),
            pltpu.VMEM((2 * cross, cross), HALF),
            pltpu.VMEM((BLOCK, cross), SINGLE),
            jax.ShapeDtypeStruct((1, LANES), SINGLE),
        ],
        scratch_shapes=[
            pltpu.VMEM((cross, cross), SINGLE),
            pltpu.VMEM((cross, cross), SINGLE),
            pltpu.VMEM((cols, cross), SINGLE),
        ],
        compiler_params=pltpu.CompilerParams(vmem_limit_bytes=VMEM_LIMIT),
        name="small_algebra",
    )(in_vmem(packed))


def right_kernel(p_ref, w_ref, phi_ref, v_ref, k_ref, u_ref, upd_ref, q_ref):
    cross = k_ref.shape[1]
    y = jnp.concatenate([phi_ref[...].astype(SINGLE), v_ref[...].astype(SINGLE)], 0).astype(HALF)
    both = jnp.dot(k_ref[...], y, preferred_element_type=SINGLE)
    q_ref[...] = (both[0:cross] + both[cross : 2 * cross]).astype(HALF)
    x = jnp.concatenate([p_ref[...].astype(SINGLE), w_ref[...].astype(SINGLE)], 0).astype(HALF)
    upd_ref[...] = jnp.sum(
        jnp.dot(u_ref[...].astype(HALF), x, preferred_element_type=SINGLE), 0, keepdims=True
    )


def right_products(p_left, w_cols, phi_right, v_cols, k_right, u):
    rank, local = p_left.shape
    cols = w_cols.shape[0]
    cross = rank + cols
    wide = min(local, 2048)
    spec = lambda rows: pl.BlockSpec((rows, wide), lambda i: (0, i))
    return pl.pallas_call(
        right_kernel,
        grid=(local // wide,),
        in_specs=[
            spec(rank), spec(cols), spec(rank), spec(cols),
            pl.BlockSpec((2 * cross, cross), lambda i: (0, 0)),
            pl.BlockSpec((BLOCK, cross), lambda i: (0, 0)),
        ],
        out_specs=[spec(1), spec(cross)],
        out_shape=[
            jax.ShapeDtypeStruct((1, local), SINGLE),
            pltpu.HBM((cross, local), HALF),
        ],
        compiler_params=pltpu.CompilerParams(vmem_limit_bytes=VMEM_LIMIT),
        name="right_products",
    )(*in_hbm(p_left, w_cols, phi_right, v_cols), in_vmem(k_right), in_vmem(u))


def left_kernel(x_ref, k_ref, q_ref, ready, sem):
    n, cross, share = x_ref.shape
    group = n // sem.shape[0]
    wide = group * share
    k = k_ref[...]
    copies = []
    for at in range(sem.shape[0]):
        for i in range(group):
            both = jnp.dot(k, x_ref[at * group + i], preferred_element_type=SINGLE)
            ready[:, at * wide + i * share : at * wide + (i + 1) * share] = (
                both[0:cross] + both[cross : 2 * cross]
            ).astype(HALF)
        cut = pl.ds(at * wide, wide)
        copies.append(pltpu.make_async_copy(ready.at[:, cut], q_ref.at[:, cut], sem.at[at]))
        copies[-1].start()
    for copy in copies:
        copy.wait()


def left_products(sorted_x, k_left):
    n, cross, share = sorted_x.shape
    group = max(1, 512 // share)
    vmem = pl.BlockSpec(memory_space=pltpu.VMEM)
    return pl.pallas_call(
        left_kernel,
        in_specs=[vmem, vmem],
        out_specs=pl.BlockSpec(memory_space=pltpu.HBM),
        out_shape=pltpu.HBM((cross, n * share), HALF),
        scratch_shapes=[
            pltpu.VMEM((cross, n * share), HALF),
            pltpu.SemaphoreType.DMA((n // group,)),
        ],
        compiler_params=pltpu.CompilerParams(vmem_limit_bytes=VMEM_LIMIT),
        name="left_products",
    )(in_vmem(sorted_x), in_vmem(k_left))


def swap(x, reach):
    n = lax.axis_size("rows")
    return lax.ppermute(x, "rows", [(i, i ^ reach) for i in range(n)])


def split(x, reach):
    half = x.shape[0] // 2
    bit = lax.rem(lax.div(lax.axis_index("rows"), reach), 2)
    kept = lax.dynamic_slice_in_dim(x, bit * half, half)
    given = lax.dynamic_slice_in_dim(x, (1 - bit) * half, half)
    return kept + swap(given, reach)


def join(x, reach):
    bit = lax.rem(lax.div(lax.axis_index("rows"), reach), 2)
    other = swap(x, reach)
    return jnp.where(bit == 0, jnp.concatenate([x, other], 0), jnp.concatenate([other, x], 0))


def shards(p_left, phi_right, v_cols, w_cols, residual):
    rank, local = p_left.shape
    cols = v_cols.shape[0]
    n = lax.axis_size("rows")
    near = [1 << i for i in range(3)]
    far = [1 << i for i in range(3, n.bit_length() - 1)]
    packed, x = packed_grams(p_left, w_cols, phi_right, v_cols, residual)
    mine = sort_by_owner(x, n)
    for reach in far[:-1]:
        packed = packed + swap(packed, reach)
    mine, packed = lax.optimization_barrier((mine, packed))
    other = swap(packed, far[-1])
    owned = lax.all_to_all(mine, "rows", split_axis=0, concat_axis=0, tiled=True)
    packed = packed + other
    packed = split(packed, near[0])
    for reach in near[1:]:
        packed = packed + swap(packed, reach)
    packed = join(packed, near[0])
    k_left, k_right, u, rms = small_algebra(packed, rank, cols, float(local * n))
    update, q_right = right_products(p_left, w_cols, phi_right, v_cols, k_right, u)
    q_left = left_products(owned, k_left)
    return (update.reshape(local), q_left, q_right, rms[0, 0:2])


def solution(mesh):
    placed = (P(None, "rows"), P(None, "rows"), P(None, "rows"), P(None, "rows"), P("rows"))
    return jax.shard_map(
        shards,
        mesh=mesh,
        in_specs=placed,
        out_specs=(P("rows"), P(None, "rows"), P(None, "rows"), P()),
        check_vma=False,
    )
```

```python
import functools

import jax
import jax.numpy as jnp
from jax import lax
from jax.experimental import pallas as pl
from jax.experimental.pallas import tpu as pltpu
from jax.sharding import PartitionSpec as P

SINGLE = jnp.float32
HALF = jnp.bfloat16
LANES = 128
BLOCK = 8
HIGHEST = lax.Precision.HIGHEST
NT = (((1,), (1,)), ((), ()))
VMEM_LIMIT = 24 * 1024 * 1024
SORT_TILE = 256


def iota(shape, dim):
    return lax.broadcasted_iota(jnp.int32, shape, dim)


def dot_hi(a, b, dims=None):
    if dims is None:
        return jnp.dot(a, b, precision=HIGHEST, preferred_element_type=SINGLE)
    return lax.dot_general(a, b, dims, precision=HIGHEST, preferred_element_type=SINGLE)


def in_vmem(x):
    return pltpu.with_memory_space_constraint(x, pltpu.VMEM)


def in_hbm(*xs):
    return [pltpu.with_memory_space_constraint(x, pltpu.HBM) for x in xs]


def to_half(x):
    return x.astype(HALF).astype(SINGLE)


def sort_kernel(n, x_ref, out_ref, turned, ready, sem):
    cross, local = x_ref.shape
    tile = SORT_TILE
    runs = tile // n
    row, column = iota((tile, tile), 0), iota((tile, tile), 1)
    wanted = lax.rem(row, runs) * n + lax.div(row, runs)
    permutation = jnp.where(column == wanted, 1.0, 0.0).astype(HALF)
    pair = 16 // runs if runs < 16 else 1
    for at in range(0, local, tile * pair):
        parts = []
        for i in range(pair):
            x = x_ref[:, at + i * tile : at + (i + 1) * tile]
            part = lax.dot_general(permutation, x, NT, preferred_element_type=SINGLE)
            parts.append(part.reshape(n, runs, cross))
        rows = slice(at // n, at // n + runs * pair)
        turned[:, rows, :] = jnp.concatenate(parts, 1).astype(HALF)
    copies = []
    for owner in range(n):
        ready[owner] = turned[owner].T
        copies.append(pltpu.make_async_copy(ready.at[owner], out_ref.at[owner], sem.at[owner]))
        if owner:
            copies[-2].start()
    copies[-1].start()
    for copy in copies:
        copy.wait()


def sort_by_owner(x, n):
    cross, local = x.shape
    share = local // n
    return pl.pallas_call(
        functools.partial(sort_kernel, n),
        in_specs=[pl.BlockSpec(memory_space=pltpu.VMEM)],
        out_specs=pl.BlockSpec(memory_space=pltpu.HBM),
        out_shape=pltpu.HBM((n, cross, share), HALF),
        scratch_shapes=[
            pltpu.VMEM((n, share, cross), HALF),
            pltpu.VMEM((n, cross, share), HALF),
            pltpu.SemaphoreType.DMA((n,)),
        ],
        compiler_params=pltpu.CompilerParams(vmem_limit_bytes=VMEM_LIMIT),
        name="sort_by_owner",
    )(in_vmem(x))


def gram_kernel(chunks, p_hbm, w_hbm, phi_hbm, v_hbm, res_hbm, out_ref, x_ref, *scratch):
    *buffers, left, right, sem = scratch
    sources = (p_hbm, w_hbm, phi_hbm, v_hbm)
    wide = x_ref.shape[1] // chunks
    res_buffer = buffers[-1]
    res_copy = pltpu.make_async_copy(res_hbm, res_buffer, sem.at[len(sources), 0])
    copies = []
    for at in range(chunks):
        cut = pl.ds(at * wide, wide)
        copies.append(
            [
                pltpu.make_async_copy(source.at[:, cut], buffer.at[:, cut], sem.at[i, at])
                for i, (source, buffer) in enumerate(zip(sources, buffers))
            ]
        )
        for copy in copies[-1]:
            copy.start()
        if at == 0:
            res_copy.start()
    for at in range(chunks):
        cut = slice(at * wide, (at + 1) * wide)
        for copy in copies[at]:
            copy.wait()
        if at == 0:
            res_copy.wait()
        p, w, phi, v = [buffer[:, cut].astype(SINGLE) for buffer in buffers[:4]]
        x = jnp.concatenate([p, w], 0).astype(HALF)
        x_ref[:, cut] = x
        more = lax.dot_general(x, x, NT, preferred_element_type=SINGLE)
        left[...] = more if at == 0 else left[...] + more
        y = jnp.concatenate([phi, v], 0).astype(HALF)
        res = res_buffer[cut].astype(SINGLE).reshape(1, wide)
        last = jnp.where(iota((16, wide), 0) == 0, res, 0.0).astype(HALF)
        z = jnp.concatenate([y, last], 0)
        more = lax.dot_general(z, z, NT, preferred_element_type=SINGLE)
        right[...] = more if at == 0 else right[...] + more
    cross = left.shape[0]
    m = LANES
    e = cross - m
    top_right = right[0:m, 0:m]
    same = iota((m, m), 0) == iota((m, m), 1)
    out_ref[0:m, :] = jnp.where(iota((m, m), 1) <= iota((m, m), 0), left[0:m, 0:m], top_right)
    out_ref[m : m + e, :] = left[m:cross, 0:m]
    out_ref[m + e : m + 2 * e, :] = right[m:cross, 0:m]
    corner_right = right[m:cross, m:cross]
    lower = iota((e, e), 1) <= iota((e, e), 0)
    corner = jnp.where(lower, left[m:cross, m:cross], corner_right)
    base = m + 2 * e
    out_ref[base : base + 2 * BLOCK, :] = jnp.zeros((2 * BLOCK, m), SINGLE)
    for i in range(e // BLOCK):
        out_ref[base : base + BLOCK, i * e : (i + 1) * e] = corner[i * BLOCK : (i + 1) * BLOCK, :]
    base += BLOCK
    out_ref[base : base + 1, :] = jnp.sum(jnp.where(same, top_right, 0.0), 0, keepdims=True)
    out_ref[base + 1 : base + 2, :] = right[cross : cross + 1, 0:m]
    out_ref[base + 2 : base + 3, 0 : e + 1] = right[cross : cross + 1, m : cross + 1]
    out_ref[base + 3 : base + 4, 0:e] = jnp.sum(
        jnp.where(iota((e, e), 0) == iota((e, e), 1), corner_right, 0.0), 0, keepdims=True
    )


def packed_rows(cross):
    return LANES + 2 * (cross - LANES) + 2 * BLOCK


def packed_grams(p_left, w_cols, phi_right, v_cols, residual):
    rank, local = p_left.shape
    cols = w_cols.shape[0]
    cross = rank + cols
    chunks = 2
    hbm = pl.BlockSpec(memory_space=pltpu.HBM)
    vmem = pl.BlockSpec(memory_space=pltpu.VMEM)
    return pl.pallas_call(
        functools.partial(gram_kernel, chunks),
        in_specs=[hbm] * 5,
        out_specs=[vmem] * 2,
        out_shape=[
            pltpu.VMEM((packed_rows(cross), LANES), SINGLE),
            pltpu.VMEM((cross, local), HALF),
        ],
        scratch_shapes=[
            pltpu.VMEM((rank, local), HALF),
            pltpu.VMEM((cols, local), HALF),
            pltpu.VMEM((rank, local), HALF),
            pltpu.VMEM((cols, local), HALF),
            pltpu.VMEM((local,), HALF),
            pltpu.VMEM((cross, cross), SINGLE),
            pltpu.VMEM((cross + 16, cross + 16), SINGLE),
            pltpu.SemaphoreType.DMA((5, chunks)),
        ],
        compiler_params=pltpu.CompilerParams(vmem_limit_bytes=VMEM_LIMIT),
        name="packed_grams",
    )(*in_hbm(p_left, w_cols, phi_right, v_cols, residual))


def eliminate(refs, tops, k):
    panels = []
    for ref, top in zip(refs, tops):
        cross = ref.shape[1]
        x = ref[pl.ds(pl.multiple_of(k - top, BLOCK), BLOCK), :]
        lane, sub = iota((BLOCK, cross), 1), iota((BLOCK, cross), 0)
        column = [
            jnp.sum(jnp.where(lane == k + i, x, 0.0), 1, keepdims=True) for i in range(BLOCK)
        ]
        rel = lane - k
        x = jnp.where((rel >= 0) & (rel < BLOCK), jnp.where(rel == sub, 1.0, 0.0), x)
        panels.append([x, column, rel, sub])
    thin = iota((BLOCK, 1), 0)
    for i in range(BLOCK):
        for panel in panels:
            x, column, rel, sub = panel
            scale = lax.rsqrt(column[i][i : i + 1, :])
            factor = jnp.where(thin > i, column[i] * scale, 0.0)
            for j in range(i + 1, BLOCK):
                column[j] = column[j] - factor * (column[j][i : i + 1, :] * scale)
            row = x[i : i + 1, :] * scale
            panel[0] = jnp.where(sub == i, row, x - factor * row)
    for ref, top, (x, _, rel, _) in zip(refs, tops, panels):
        cross = ref.shape[1]
        right = jnp.where(rel >= BLOCK, x, 0.0)
        done = jnp.where(rel < BLOCK, x, 0.0)
        r0 = to_half(right)
        r1 = to_half(right - r0)
        r2 = right - r0 - r1
        x0 = to_half(x)
        x1 = to_half(x - x0)
        x2 = x - x0 - x1
        lhs = jnp.concatenate([r0, r0, r0, r1, r1, r2], 0)
        if top:
            lhs = jnp.concatenate([lhs, jnp.zeros((LANES - lhs.shape[0], cross), SINGLE)], 0)
            lhs = lhs.T[top:cross, 0 : 6 * BLOCK].astype(HALF)
        else:
            lhs = lhs.T.astype(HALF)
        rhs = jnp.concatenate([x0, x1, x2, x0, x1, x0], 0).astype(HALF)
        change = jnp.dot(lhs, rhs, preferred_element_type=SINGLE)
        here = iota(ref.shape, 1) - k
        ref[...] = jnp.where((here >= 0) & (here < BLOCK), 0.0, ref[...]) - change
        ref[pl.ds(pl.multiple_of(k - top, BLOCK), BLOCK), :] = done


def small_kernel(rank, count, g_ref, top_ref, low_ref, kr_ref, u_ref, rms_ref, left, right, tail):
    cross = left.shape[0]
    m = LANES
    e = cross - m
    base = m + 2 * e + BLOCK

    def unfold(packed, diagonal):
        rows, lanes = iota(packed.shape, 0), iota(packed.shape, 1)
        lower = jnp.where(lanes < rows, packed, 0.0)
        upper = jnp.where(lanes > rows, packed, 0.0)
        same = rows == lanes
        return (
            lower + lower.T + jnp.where(same, packed, 0.0),
            upper + upper.T + jnp.where(same, diagonal, 0.0),
        )

    left[0:m, 0:m], right[0:m, 0:m] = unfold(g_ref[0:m, :], g_ref[base : base + 1, :])
    left[m:cross, 0:m] = g_ref[m : m + e, :]
    right[m:cross, 0:m] = g_ref[m + e : m + 2 * e, :]
    left[0:m, m:cross] = g_ref[m : m + e, :].T
    right[0:m, m:cross] = g_ref[m + e : m + 2 * e, :].T
    corner = jnp.concatenate(
        [g_ref[base - BLOCK : base, i * e : (i + 1) * e] for i in range(e // BLOCK)], 0
    )
    left[m:cross, m:cross], right[m:cross, m:cross] = unfold(corner, g_ref[base + 3 : base + 4, 0:e])
    g_left = left[...]
    g_right = right[...]
    res_first = g_ref[base + 1 : base + 2, :]
    res_rest = g_ref[base + 2 : base + 3, 0:e]
    res_row = jnp.concatenate([res_first, res_rest], 1)
    res_sq = g_ref[base + 2 : base + 3, e : e + 1]

    tail[...] = g_right[rank:cross, :]
    lax.fori_loop(
        rank // BLOCK, cross // BLOCK, lambda b, c: (eliminate([tail], [rank], b * BLOCK), c)[1], 0
    )
    low_lane = iota((cross - rank, cross), 1)
    low_row = iota((cross - rank, cross), 0)
    inverse = jnp.where(low_lane >= rank, tail[...], 0.0)
    eye = jnp.where(iota((rank, cross), 0) == iota((rank, cross), 1), 1.0, 0.0)

    mix = jnp.where(
        low_lane < rank, -to_half(g_right[rank:cross, :]), jnp.where(low_lane == low_row + rank, 1.0, 0.0)
    )
    to_tilde = jnp.concatenate([eye, mix], 0)
    t_right = jnp.concatenate([eye, inverse], 0)
    t_left = jnp.concatenate([eye, dot_hi(inverse, to_tilde)], 0)

    lane8 = iota((BLOCK, cross), 1)
    res8 = jnp.broadcast_to(res_row, (BLOCK, cross))
    half_way = dot_hi(jnp.where(lane8 >= rank, res8, 0.0), inverse, NT)
    coeffs = -dot_hi(half_way, inverse)
    u = dot_hi(jnp.where(lane8 < rank, -to_half(res8), coeffs), to_tilde)
    upd_sq = jnp.sum(dot_hi(u, g_left) * u, 1, keepdims=True)[0:1, :]
    u0 = to_half(u)
    u1 = to_half(u - u0)
    u2 = u - u0 - u1
    sub8 = iota((BLOCK, cross), 0)
    u_ref[...] = jnp.where(sub8 == 0, u0, jnp.where(sub8 == 1, u1, jnp.where(sub8 == 2, u2, 0.0)))
    lane_out = iota((1, LANES), 1)
    rms_ref[...] = jnp.sqrt(jnp.where(lane_out == 0, res_sq, upd_sq) / count)

    left[...] = dot_hi(dot_hi(t_left, g_left), t_left, NT)
    right[...] = dot_hi(dot_hi(t_right, g_right), t_right, NT)
    lax.fori_loop(
        0, cross // BLOCK, lambda b, c: (eliminate([left, right], [0, 0], b * BLOCK), c)[1], 0
    )
    k = dot_hi(left[...], t_left)
    k0 = to_half(k)
    k1 = k - k0
    top_ref[:, 0:m] = k0[0:m, 0:m].astype(HALF)
    top_ref[:, m : 2 * m] = k1[0:m, 0:m].astype(HALF)
    low_ref[0:e, :] = k0[m:cross, :].astype(HALF)
    low_ref[e : 2 * e, :] = k1[m:cross, :].astype(HALF)
    k = dot_hi(right[...], t_right)
    k0 = to_half(k)
    kr_ref[0:cross, :] = k0.astype(HALF)
    kr_ref[cross : 2 * cross, :] = (k - k0).astype(HALF)


def small_algebra(packed, rank, cols, count):
    cross = rank + cols
    vmem = pl.BlockSpec(memory_space=pltpu.VMEM)
    return pl.pallas_call(
        functools.partial(small_kernel, rank, count),
        in_specs=[vmem],
        out_specs=[vmem] * 5,
        out_shape=[
            pltpu.VMEM((LANES, 2 * LANES), HALF),
            pltpu.VMEM((2 * (cross - LANES), cross), HALF),
            pltpu.VMEM((2 * cross, cross), HALF),
            pltpu.VMEM((BLOCK, cross), SINGLE),
            jax.ShapeDtypeStruct((1, LANES), SINGLE),
        ],
        scratch_shapes=[
            pltpu.VMEM((cross, cross), SINGLE),
            pltpu.VMEM((cross, cross), SINGLE),
            pltpu.VMEM((cols, cross), SINGLE),
        ],
        compiler_params=pltpu.CompilerParams(vmem_limit_bytes=VMEM_LIMIT),
        name="small_algebra",
    )(in_vmem(packed))


def right_kernel(p_ref, w_ref, phi_ref, v_ref, k_ref, u_ref, upd_ref, q_ref):
    cross = k_ref.shape[1]
    y = jnp.concatenate([phi_ref[...].astype(SINGLE), v_ref[...].astype(SINGLE)], 0).astype(HALF)
    both = jnp.dot(k_ref[...], y, preferred_element_type=SINGLE)
    q_ref[...] = (both[0:cross] + both[cross : 2 * cross]).astype(HALF)
    x = jnp.concatenate([p_ref[...].astype(SINGLE), w_ref[...].astype(SINGLE)], 0).astype(HALF)
    upd_ref[...] = jnp.sum(
        jnp.dot(u_ref[...].astype(HALF), x, preferred_element_type=SINGLE), 0, keepdims=True
    )


def right_products(p_left, w_cols, phi_right, v_cols, k_right, u):
    rank, local = p_left.shape
    cols = w_cols.shape[0]
    cross = rank + cols
    wide = min(local, 2048)
    spec = lambda rows: pl.BlockSpec((rows, wide), lambda i: (0, i))
    return pl.pallas_call(
        right_kernel,
        grid=(local // wide,),
        in_specs=[
            spec(rank), spec(cols), spec(rank), spec(cols),
            pl.BlockSpec((2 * cross, cross), lambda i: (0, 0)),
            pl.BlockSpec((BLOCK, cross), lambda i: (0, 0)),
        ],
        out_specs=[spec(1), spec(cross)],
        out_shape=[
            jax.ShapeDtypeStruct((1, local), SINGLE),
            pltpu.HBM((cross, local), HALF),
        ],
        compiler_params=pltpu.CompilerParams(vmem_limit_bytes=VMEM_LIMIT),
        name="right_products",
    )(*in_hbm(p_left, w_cols, phi_right, v_cols), in_vmem(k_right), in_vmem(u))


def left_kernel(x_ref, top_ref, low_ref, q_ref, ready, sem):
    n, cross, share = x_ref.shape
    m = LANES
    e = cross - m
    group = n // sem.shape[0]
    wide = group * share
    copies = []
    for at in range(sem.shape[0]):
        for i in range(group):
            x = x_ref[at * group + i]
            cut = slice(at * wide + i * share, at * wide + (i + 1) * share)
            twice = jnp.concatenate([x[0:m], x[0:m]], 0)
            ready[0:m, cut] = jnp.dot(top_ref[...], twice, preferred_element_type=SINGLE).astype(HALF)
            low = jnp.dot(low_ref[...], x, preferred_element_type=SINGLE)
            ready[m:cross, cut] = (low[0:e] + low[e : 2 * e]).astype(HALF)
        cut = pl.ds(at * wide, wide)
        copies.append(pltpu.make_async_copy(ready.at[:, cut], q_ref.at[:, cut], sem.at[at]))
        if at:
            copies[-2].start()
    copies[-1].start()
    for copy in copies:
        copy.wait()


def left_products(sorted_x, top, low):
    n, cross, share = sorted_x.shape
    group = max(1, 512 // share)
    vmem = pl.BlockSpec(memory_space=pltpu.VMEM)
    return pl.pallas_call(
        left_kernel,
        in_specs=[vmem, vmem, vmem],
        out_specs=pl.BlockSpec(memory_space=pltpu.HBM),
        out_shape=pltpu.HBM((cross, n * share), HALF),
        scratch_shapes=[
            pltpu.VMEM((cross, n * share), HALF),
            pltpu.SemaphoreType.DMA((n // group,)),
        ],
        compiler_params=pltpu.CompilerParams(vmem_limit_bytes=VMEM_LIMIT),
        name="left_products",
    )(in_vmem(sorted_x), in_vmem(top), in_vmem(low))


def swap(x, reach):
    n = lax.axis_size("rows")
    return lax.ppermute(x, "rows", [(i, i ^ reach) for i in range(n)])


def split(x, reach):
    half = x.shape[0] // 2
    bit = lax.rem(lax.div(lax.axis_index("rows"), reach), 2)
    kept = lax.dynamic_slice_in_dim(x, bit * half, half)
    given = lax.dynamic_slice_in_dim(x, (1 - bit) * half, half)
    return kept + swap(given, reach)


def join(x, reach):
    bit = lax.rem(lax.div(lax.axis_index("rows"), reach), 2)
    other = swap(x, reach)
    return jnp.where(bit == 0, jnp.concatenate([x, other], 0), jnp.concatenate([other, x], 0))


def shards(p_left, phi_right, v_cols, w_cols, residual):
    rank, local = p_left.shape
    cols = v_cols.shape[0]
    n = lax.axis_size("rows")
    near = [1 << i for i in range(3)]
    far = [1 << i for i in range(3, n.bit_length() - 1)]
    packed, x = packed_grams(p_left, w_cols, phi_right, v_cols, residual)
    mine = sort_by_owner(x, n)
    for reach in far[:-1]:
        packed = packed + swap(packed, reach)
    mine, packed = lax.optimization_barrier((mine, packed))
    other = swap(packed, far[-1])
    owned = lax.all_to_all(mine, "rows", split_axis=0, concat_axis=0, tiled=True)
    packed = packed + other
    packed = split(packed, near[0])
    for reach in near[1:]:
        packed = packed + swap(packed, reach)
    packed = join(packed, near[0])
    k_top, k_low, k_right, u, rms = small_algebra(packed, rank, cols, float(local * n))
    update, q_right = right_products(p_left, w_cols, phi_right, v_cols, k_right, u)
    q_left = left_products(owned, k_top, k_low)
    return (update.reshape(local), q_left, q_right, rms[0, 0:2])


def solution(mesh):
    placed = (P(None, "rows"), P(None, "rows"), P(None, "rows"), P(None, "rows"), P("rows"))
    return jax.shard_map(
        shards,
        mesh=mesh,
        in_specs=placed,
        out_specs=(P("rows"), P(None, "rows"), P(None, "rows"), P()),
        check_vma=False,
    )
```

```python
import functools

import jax
import jax.numpy as jnp
from jax import lax
from jax.experimental import pallas as pl
from jax.experimental.pallas import tpu as pltpu
from jax.sharding import PartitionSpec as P

SINGLE = jnp.float32
HALF = jnp.bfloat16
LANES = 128
BLOCK = 8
HIGHEST = lax.Precision.HIGHEST
NT = (((1,), (1,)), ((), ()))
VMEM_LIMIT = 24 * 1024 * 1024
SORT_TILE = 256


def iota(shape, dim):
    return lax.broadcasted_iota(jnp.int32, shape, dim)


def dot_hi(a, b, dims=None):
    if dims is None:
        return jnp.dot(a, b, precision=HIGHEST, preferred_element_type=SINGLE)
    return lax.dot_general(a, b, dims, precision=HIGHEST, preferred_element_type=SINGLE)


def in_vmem(x):
    return pltpu.with_memory_space_constraint(x, pltpu.VMEM)


def in_hbm(*xs):
    return [pltpu.with_memory_space_constraint(x, pltpu.HBM) for x in xs]


def to_half(x):
    return x.astype(HALF).astype(SINGLE)


def sort_kernel(n, x_ref, out_ref, turned, ready, sem):
    cross, local = x_ref.shape
    tile = SORT_TILE
    runs = tile // n
    row, column = iota((tile, tile), 0), iota((tile, tile), 1)
    wanted = lax.rem(row, runs) * n + lax.div(row, runs)
    permutation = jnp.where(column == wanted, 1.0, 0.0).astype(HALF)
    pair = 16 // runs if runs < 16 else 1
    for at in range(0, local, tile * pair):
        parts = []
        for i in range(pair):
            x = x_ref[:, at + i * tile : at + (i + 1) * tile]
            part = lax.dot_general(permutation, x, NT, preferred_element_type=SINGLE)
            parts.append(part.reshape(n, runs, cross))
        rows = slice(at // n, at // n + runs * pair)
        turned[:, rows, :] = jnp.concatenate(parts, 1).astype(HALF)
    copies = []
    for owner in range(n):
        ready[owner] = turned[owner].T
        copies.append(pltpu.make_async_copy(ready.at[owner], out_ref.at[owner], sem.at[owner]))
        if owner:
            copies[-2].start()
    copies[-1].start()
    for copy in copies:
        copy.wait()


def sort_by_owner(x, n):
    cross, local = x.shape
    share = local // n
    return pl.pallas_call(
        functools.partial(sort_kernel, n),
        in_specs=[pl.BlockSpec(memory_space=pltpu.VMEM)],
        out_specs=pl.BlockSpec(memory_space=pltpu.HBM),
        out_shape=pltpu.HBM((n, cross, share), HALF),
        scratch_shapes=[
            pltpu.VMEM((n, share, cross), HALF),
            pltpu.VMEM((n, cross, share), HALF),
            pltpu.SemaphoreType.DMA((n,)),
        ],
        compiler_params=pltpu.CompilerParams(vmem_limit_bytes=VMEM_LIMIT),
        name="sort_by_owner",
    )(in_vmem(x))


def gram_kernel(chunks, p_hbm, w_hbm, phi_hbm, v_hbm, res_hbm, out_ref, x_ref, *scratch):
    *buffers, left, right, sem = scratch
    sources = (p_hbm, w_hbm, phi_hbm, v_hbm)
    wide = x_ref.shape[1] // chunks
    res_buffer = buffers[-1]
    res_copy = pltpu.make_async_copy(res_hbm, res_buffer, sem.at[len(sources), 0])
    copies = []
    for at in range(chunks):
        cut = pl.ds(at * wide, wide)
        copies.append(
            [
                pltpu.make_async_copy(source.at[:, cut], buffer.at[:, cut], sem.at[i, at])
                for i, (source, buffer) in enumerate(zip(sources, buffers))
            ]
        )
        for copy in copies[-1]:
            copy.start()
        if at == 0:
            res_copy.start()
    for at in range(chunks):
        cut = slice(at * wide, (at + 1) * wide)
        for copy in copies[at]:
            copy.wait()
        if at == 0:
            res_copy.wait()
        p, w, phi, v = [buffer[:, cut].astype(SINGLE) for buffer in buffers[:4]]
        x = jnp.concatenate([p, w], 0).astype(HALF)
        x_ref[:, cut] = x
        more = lax.dot_general(x, x, NT, preferred_element_type=SINGLE)
        left[...] = more if at == 0 else left[...] + more
        y = jnp.concatenate([phi, v], 0).astype(HALF)
        res = res_buffer[cut].astype(SINGLE).reshape(1, wide)
        last = jnp.where(iota((16, wide), 0) == 0, res, 0.0).astype(HALF)
        z = jnp.concatenate([y, last], 0)
        more = lax.dot_general(z, z, NT, preferred_element_type=SINGLE)
        right[...] = more if at == 0 else right[...] + more
    cross = left.shape[0]
    m = LANES
    e = cross - m
    top_right = right[0:m, 0:m]
    same = iota((m, m), 0) == iota((m, m), 1)
    out_ref[0:m, :] = jnp.where(iota((m, m), 1) <= iota((m, m), 0), left[0:m, 0:m], top_right)
    out_ref[m : m + e, :] = left[m:cross, 0:m]
    out_ref[m + e : m + 2 * e, :] = right[m:cross, 0:m]
    corner_right = right[m:cross, m:cross]
    lower = iota((e, e), 1) <= iota((e, e), 0)
    corner = jnp.where(lower, left[m:cross, m:cross], corner_right)
    base = m + 2 * e
    out_ref[base : base + 2 * BLOCK, :] = jnp.zeros((2 * BLOCK, m), SINGLE)
    for i in range(e // BLOCK):
        out_ref[base : base + BLOCK, i * e : (i + 1) * e] = corner[i * BLOCK : (i + 1) * BLOCK, :]
    base += BLOCK
    out_ref[base : base + 1, :] = jnp.sum(jnp.where(same, top_right, 0.0), 0, keepdims=True)
    out_ref[base + 1 : base + 2, :] = right[cross : cross + 1, 0:m]
    out_ref[base + 2 : base + 3, 0 : e + 1] = right[cross : cross + 1, m : cross + 1]
    out_ref[base + 3 : base + 4, 0:e] = jnp.sum(
        jnp.where(iota((e, e), 0) == iota((e, e), 1), corner_right, 0.0), 0, keepdims=True
    )


def packed_rows(cross):
    return LANES + 2 * (cross - LANES) + 2 * BLOCK


def packed_grams(p_left, w_cols, phi_right, v_cols, residual):
    rank, local = p_left.shape
    cols = w_cols.shape[0]
    cross = rank + cols
    chunks = 2
    hbm = pl.BlockSpec(memory_space=pltpu.HBM)
    vmem = pl.BlockSpec(memory_space=pltpu.VMEM)
    return pl.pallas_call(
        functools.partial(gram_kernel, chunks),
        in_specs=[hbm] * 5,
        out_specs=[vmem] * 2,
        out_shape=[
            pltpu.VMEM((packed_rows(cross), LANES), SINGLE),
            pltpu.VMEM((cross, local), HALF),
        ],
        scratch_shapes=[
            pltpu.VMEM((rank, local), HALF),
            pltpu.VMEM((cols, local), HALF),
            pltpu.VMEM((rank, local), HALF),
            pltpu.VMEM((cols, local), HALF),
            pltpu.VMEM((local,), HALF),
            pltpu.VMEM((cross, cross), SINGLE),
            pltpu.VMEM((cross + 16, cross + 16), SINGLE),
            pltpu.SemaphoreType.DMA((5, chunks)),
        ],
        compiler_params=pltpu.CompilerParams(vmem_limit_bytes=VMEM_LIMIT),
        name="packed_grams",
    )(*in_hbm(p_left, w_cols, phi_right, v_cols, residual))


def eliminate(refs, tops):
    crosses = [ref.shape[1] for ref in refs]
    steps = refs[0].shape[0] // BLOCK
    lane, sub = [iota((BLOCK, cross), 1) for cross in crosses], [iota((BLOCK, cross), 0) for cross in crosses]
    thin = iota((BLOCK, 1), 0)

    def step(at, carry):
        row_at = pl.multiple_of(at * BLOCK, BLOCK)
        panels, befores = carry
        for ref, top, x, lanes, cross in zip(refs, tops, befores, lane, crosses):
            far = jnp.where(lanes - (row_at + top) >= BLOCK, x, 0.0)
            r0 = to_half(far)
            r1 = to_half(far - r0)
            r2 = far - r0 - r1
            x0 = to_half(x)
            x1 = to_half(x - x0)
            x2 = x - x0 - x1
            lhs = jnp.concatenate([r0, r0, r0, r1, r1, r2] + [jnp.zeros_like(x)] * 10, 0)
            lhs = lhs.T[top:cross, 0 : 6 * BLOCK].astype(HALF)
            rhs = jnp.concatenate([x0, x1, x2, x0, x1, x0], 0).astype(HALF)
            change = jnp.dot(lhs, rhs, preferred_element_type=SINGLE)
            here = iota(ref.shape, 1) - (row_at + top) + BLOCK
            later = iota(ref.shape, 0) >= row_at + BLOCK
            ref[...] = jnp.where((here >= 0) & (here < BLOCK) & later, 0.0, ref[...]) - change
        columns, scaled = [], []
        for x, top, lanes, subs in zip(panels, tops, lane, sub):
            rel = lanes - (row_at + top)
            columns.append([jnp.sum(jnp.where(rel == i, x, 0.0), 1, keepdims=True) for i in range(BLOCK)])
            scaled.append(jnp.where((rel >= 0) & (rel < BLOCK), jnp.where(rel == subs, 1.0, 0.0), x))
        for i in range(BLOCK):
            for which, column in enumerate(columns):
                scale = lax.rsqrt(column[i][i : i + 1, :])
                factor = jnp.where(thin > i, column[i] * scale, 0.0)
                for j in range(i + 1, BLOCK):
                    column[j] = column[j] - factor * (column[j][i : i + 1, :] * scale)
                x = scaled[which]
                row = x[i : i + 1, :] * scale
                scaled[which] = jnp.where(sub[which] == i, row, x - factor * row)
        nexts = []
        for ref, top, x, lanes, subs in zip(refs, tops, scaled, lane, sub):
            rel = lanes - (row_at + top)
            ref[pl.ds(row_at, BLOCK), :] = jnp.where(rel < BLOCK, x, 0.0)
            ahead = pl.multiple_of(lax.rem(row_at + BLOCK, ref.shape[0]), BLOCK)
            rows = jnp.where((rel >= 0) & (rel < BLOCK), 0.0, ref[pl.ds(ahead, BLOCK), :])
            for i in range(BLOCK):
                row = x[i : i + 1, :]
                weight = jnp.sum(jnp.where(rel == subs + BLOCK, row, 0.0), 1, keepdims=True)
                rows = rows - weight * row
            nexts.append(rows)
        return nexts, scaled

    starts = [ref[0:BLOCK, :] for ref in refs]
    lax.fori_loop(0, steps, step, (starts, [jnp.zeros_like(x) for x in starts]))


def small_kernel(rank, count, g_ref, p_hbm, w_hbm, phi_hbm, v_hbm, *refs):
    top_ref, low_ref, rms_ref, upd_hbm, q_hbm, left, right, tail, *buffers, update, ready, sem, out_sem = refs
    loads = [
        pltpu.make_async_copy(source, buffer, sem.at[i])
        for i, (source, buffer) in enumerate(zip((p_hbm, w_hbm, phi_hbm, v_hbm), buffers))
    ]
    for load in loads:
        load.start()

    cross = left.shape[0]
    m = LANES
    e = cross - m
    base = m + 2 * e + BLOCK

    def unfold(packed, diagonal):
        rows, lanes = iota(packed.shape, 0), iota(packed.shape, 1)
        lower = jnp.where(lanes < rows, packed, 0.0)
        upper = jnp.where(lanes > rows, packed, 0.0)
        same = rows == lanes
        return (
            lower + lower.T + jnp.where(same, packed, 0.0),
            upper + upper.T + jnp.where(same, diagonal, 0.0),
        )

    left[0:m, 0:m], right[0:m, 0:m] = unfold(g_ref[0:m, :], g_ref[base : base + 1, :])
    left[m:cross, 0:m] = g_ref[m : m + e, :]
    right[m:cross, 0:m] = g_ref[m + e : m + 2 * e, :]
    left[0:m, m:cross] = g_ref[m : m + e, :].T
    right[0:m, m:cross] = g_ref[m + e : m + 2 * e, :].T
    corner = jnp.concatenate(
        [g_ref[base - BLOCK : base, i * e : (i + 1) * e] for i in range(e // BLOCK)], 0
    )
    left[m:cross, m:cross], right[m:cross, m:cross] = unfold(corner, g_ref[base + 3 : base + 4, 0:e])
    g_left = left[...]
    g_right = right[...]
    res_first = g_ref[base + 1 : base + 2, :]
    res_rest = g_ref[base + 2 : base + 3, 0:e]
    res_row = jnp.concatenate([res_first, res_rest], 1)
    res_sq = g_ref[base + 2 : base + 3, e : e + 1]

    tail[...] = g_right[rank:cross, :]
    eliminate([tail], [rank])
    low_lane = iota((cross - rank, cross), 1)
    low_row = iota((cross - rank, cross), 0)
    inverse = jnp.where(low_lane >= rank, tail[...], 0.0)
    eye = jnp.where(iota((rank, cross), 0) == iota((rank, cross), 1), 1.0, 0.0)

    mix = jnp.where(
        low_lane < rank, -to_half(g_right[rank:cross, :]), jnp.where(low_lane == low_row + rank, 1.0, 0.0)
    )
    to_tilde = jnp.concatenate([eye, mix], 0)
    t_right = jnp.concatenate([eye, inverse], 0)
    t_left = jnp.concatenate([eye, dot_hi(inverse, to_tilde)], 0)

    lane8 = iota((BLOCK, cross), 1)
    res8 = jnp.broadcast_to(res_row, (BLOCK, cross))
    half_way = dot_hi(jnp.where(lane8 >= rank, res8, 0.0), inverse, NT)
    coeffs = -dot_hi(half_way, inverse)
    u = dot_hi(jnp.where(lane8 < rank, -to_half(res8), coeffs), to_tilde)
    upd_sq = jnp.sum(dot_hi(u, g_left) * u, 1, keepdims=True)[0:1, :]
    u0 = to_half(u)
    u1 = to_half(u - u0)
    u2 = u - u0 - u1
    sub8 = iota((BLOCK, cross), 0)
    u = jnp.where(sub8 == 0, u0, jnp.where(sub8 == 1, u1, jnp.where(sub8 == 2, u2, 0.0))).astype(HALF)
    lane_out = iota((1, LANES), 1)
    rms_ref[...] = jnp.sqrt(jnp.where(lane_out == 0, res_sq, upd_sq) / count)

    left[...] = dot_hi(dot_hi(t_left, g_left), t_left, NT)
    right[...] = dot_hi(dot_hi(t_right, g_right), t_right, NT)
    eliminate([left, right], [0, 0])
    k = dot_hi(left[...], t_left)
    k0 = to_half(k)
    k1 = k - k0
    top_ref[:, 0:m] = k0[0:m, 0:m].astype(HALF)
    top_ref[:, m : 2 * m] = k1[0:m, 0:m].astype(HALF)
    low_ref[0:e, :] = k0[m:cross, :].astype(HALF)
    low_ref[e : 2 * e, :] = k1[m:cross, :].astype(HALF)

    k = dot_hi(right[...], t_right)
    k0 = to_half(k)
    k1 = k - k0
    k_top = jnp.concatenate([k0[0:m, 0:m], k1[0:m, 0:m]], 1).astype(HALF)
    k_low = jnp.concatenate([k0[m:cross], k1[m:cross]], 0).astype(HALF)
    for load in loads:
        load.wait()
    parts = out_sem.shape[0] - 1
    wide = ready.shape[1] // parts
    tile = 256

    def piece(at):
        cut = pl.ds(pl.multiple_of(at * wide, wide), wide)
        return pltpu.make_async_copy(ready.at[:, cut], q_hbm.at[:, cut], out_sem.at[at])

    def multiply(at, carry):
        for to in range(0, wide, tile):
            cut = pl.ds(pl.multiple_of(at * wide + to, tile), tile)
            p, w, phi, v = [buffer[:, cut].astype(SINGLE) for buffer in buffers]
            y = jnp.concatenate([phi, v], 0).astype(HALF)
            twice = jnp.concatenate([y[0:m], y[0:m]], 0)
            ready[0:m, cut] = jnp.dot(k_top, twice, preferred_element_type=SINGLE).astype(HALF)
            low = jnp.dot(k_low, y, preferred_element_type=SINGLE)
            ready[m:cross, cut] = (low[0:e] + low[e : 2 * e]).astype(HALF)
            x = jnp.concatenate([p, w], 0).astype(HALF)
            update[:, cut] = jnp.sum(jnp.dot(u, x, preferred_element_type=SINGLE), 0, keepdims=True)

        @pl.when(at > 0)
        def _():
            piece(at - 1).start()

        return carry

    lax.fori_loop(0, parts, multiply, 0)
    piece(parts - 1).start()
    whole = pltpu.make_async_copy(update, upd_hbm, out_sem.at[parts])
    whole.start()
    for at in range(parts):
        piece(at).wait()
    whole.wait()


def small_algebra(packed, p_left, w_cols, phi_right, v_cols, count):
    rank, local = p_left.shape
    cols = w_cols.shape[0]
    cross = rank + cols
    parts = 4
    vmem = pl.BlockSpec(memory_space=pltpu.VMEM)
    hbm = pl.BlockSpec(memory_space=pltpu.HBM)
    return pl.pallas_call(
        functools.partial(small_kernel, rank, count),
        in_specs=[vmem] + [hbm] * 4,
        out_specs=[vmem] * 3 + [hbm] * 2,
        out_shape=[
            pltpu.VMEM((LANES, 2 * LANES), HALF),
            pltpu.VMEM((2 * (cross - LANES), cross), HALF),
            pltpu.VMEM((1, LANES), SINGLE),
            pltpu.HBM((1, local), SINGLE),
            pltpu.HBM((cross, local), HALF),
        ],
        scratch_shapes=[
            pltpu.VMEM((cross, cross), SINGLE),
            pltpu.VMEM((cross, cross), SINGLE),
            pltpu.VMEM((cols, cross), SINGLE),
            pltpu.VMEM((rank, local), HALF),
            pltpu.VMEM((cols, local), HALF),
            pltpu.VMEM((rank, local), HALF),
            pltpu.VMEM((cols, local), HALF),
            pltpu.VMEM((1, local), SINGLE),
            pltpu.VMEM((cross, local), HALF),
            pltpu.SemaphoreType.DMA((4,)),
            pltpu.SemaphoreType.DMA((parts + 1,)),
        ],
        compiler_params=pltpu.CompilerParams(vmem_limit_bytes=VMEM_LIMIT),
        name="small_algebra",
    )(in_vmem(packed), *in_hbm(p_left, w_cols, phi_right, v_cols))


def left_kernel(x_ref, top_ref, low_ref, q_ref, ready, sem):
    n, cross, share = x_ref.shape
    m = LANES
    e = cross - m
    group = n // sem.shape[0]
    wide = group * share
    copies = []
    for at in range(sem.shape[0]):
        for i in range(group):
            x = x_ref[at * group + i]
            cut = slice(at * wide + i * share, at * wide + (i + 1) * share)
            twice = jnp.concatenate([x[0:m], x[0:m]], 0)
            ready[0:m, cut] = jnp.dot(top_ref[...], twice, preferred_element_type=SINGLE).astype(HALF)
            low = jnp.dot(low_ref[...], x, preferred_element_type=SINGLE)
            ready[m:cross, cut] = (low[0:e] + low[e : 2 * e]).astype(HALF)
        cut = pl.ds(at * wide, wide)
        copies.append(pltpu.make_async_copy(ready.at[:, cut], q_ref.at[:, cut], sem.at[at]))
        if at:
            copies[-2].start()
    copies[-1].start()
    for copy in copies:
        copy.wait()


def left_products(sorted_x, top, low):
    n, cross, share = sorted_x.shape
    group = max(1, 512 // share)
    vmem = pl.BlockSpec(memory_space=pltpu.VMEM)
    return pl.pallas_call(
        left_kernel,
        in_specs=[vmem, vmem, vmem],
        out_specs=pl.BlockSpec(memory_space=pltpu.HBM),
        out_shape=pltpu.HBM((cross, n * share), HALF),
        scratch_shapes=[
            pltpu.VMEM((cross, n * share), HALF),
            pltpu.SemaphoreType.DMA((n // group,)),
        ],
        compiler_params=pltpu.CompilerParams(vmem_limit_bytes=VMEM_LIMIT),
        name="left_products",
    )(in_vmem(sorted_x), in_vmem(top), in_vmem(low))


def swap(x, reach):
    n = lax.axis_size("rows")
    return lax.ppermute(x, "rows", [(i, i ^ reach) for i in range(n)])


def split(x, reach):
    half = x.shape[0] // 2
    bit = lax.rem(lax.div(lax.axis_index("rows"), reach), 2)
    kept = lax.dynamic_slice_in_dim(x, bit * half, half)
    given = lax.dynamic_slice_in_dim(x, (1 - bit) * half, half)
    return kept + swap(given, reach)


def join(x, reach):
    bit = lax.rem(lax.div(lax.axis_index("rows"), reach), 2)
    other = swap(x, reach)
    return jnp.where(bit == 0, jnp.concatenate([x, other], 0), jnp.concatenate([other, x], 0))


def shards(p_left, phi_right, v_cols, w_cols, residual):
    _, local = p_left.shape
    n = lax.axis_size("rows")
    near = [1 << i for i in range(3)]
    far = [1 << i for i in range(3, n.bit_length() - 1)]
    packed, x = packed_grams(p_left, w_cols, phi_right, v_cols, residual)
    mine = sort_by_owner(x, n)
    other = swap(packed, far[-1])
    owned = lax.all_to_all(mine, "rows", split_axis=0, concat_axis=0, tiled=True)
    packed = packed + other
    packed = split(packed, near[0])
    for reach in near[1:]:
        packed = packed + swap(packed, reach)
    for reach in far[:-1]:
        packed = packed + swap(packed, reach)
    packed = join(packed, near[0])
    k_top, k_low, rms, update, q_right = small_algebra(
        packed, p_left, w_cols, phi_right, v_cols, float(local * n)
    )
    q_left = left_products(owned, k_top, k_low)
    return (update.reshape(local), q_left, q_right, rms[0, 0:2])


def solution(mesh):
    placed = (P(None, "rows"), P(None, "rows"), P(None, "rows"), P(None, "rows"), P("rows"))
    return jax.shard_map(
        shards,
        mesh=mesh,
        in_specs=placed,
        out_specs=(P("rows"), P(None, "rows"), P(None, "rows"), P()),
        check_vma=False,
    )
```

```python
import functools

import jax
import jax.numpy as jnp
from jax import lax
from jax.experimental import pallas as pl
from jax.experimental.pallas import tpu as pltpu
from jax.sharding import PartitionSpec as P

SINGLE = jnp.float32
HALF = jnp.bfloat16
LANES = 128
BLOCK = 8
HIGHEST = lax.Precision.HIGHEST
NT = (((1,), (1,)), ((), ()))
VMEM_LIMIT = 24 * 1024 * 1024
SORT_TILE = 256


def iota(shape, dim):
    return lax.broadcasted_iota(jnp.int32, shape, dim)


def dot_hi(a, b, dims=None):
    if dims is None:
        return jnp.dot(a, b, precision=HIGHEST, preferred_element_type=SINGLE)
    return lax.dot_general(a, b, dims, precision=HIGHEST, preferred_element_type=SINGLE)


def in_vmem(x):
    return pltpu.with_memory_space_constraint(x, pltpu.VMEM)


def in_hbm(*xs):
    return [pltpu.with_memory_space_constraint(x, pltpu.HBM) for x in xs]


def to_half(x):
    return x.astype(HALF).astype(SINGLE)


def sort_kernel(n, x_ref, out_ref, turned, ready, sem):
    cross, local = x_ref.shape
    tile = SORT_TILE
    runs = tile // n
    row, column = iota((tile, tile), 0), iota((tile, tile), 1)
    wanted = lax.rem(row, runs) * n + lax.div(row, runs)
    permutation = jnp.where(column == wanted, 1.0, 0.0).astype(HALF)
    pair = 16 // runs if runs < 16 else 1
    for at in range(0, local, tile * pair):
        parts = []
        for i in range(pair):
            x = x_ref[:, at + i * tile : at + (i + 1) * tile]
            part = lax.dot_general(permutation, x, NT, preferred_element_type=SINGLE)
            parts.append(part.reshape(n, runs, cross))
        rows = slice(at // n, at // n + runs * pair)
        turned[:, rows, :] = jnp.concatenate(parts, 1).astype(HALF)
    copies = []
    for owner in range(n):
        ready[owner] = turned[owner].T
        copies.append(pltpu.make_async_copy(ready.at[owner], out_ref.at[owner], sem.at[owner]))
        if owner:
            copies[-2].start()
    copies[-1].start()
    for copy in copies:
        copy.wait()


def sort_by_owner(x, n):
    cross, local = x.shape
    share = local // n
    return pl.pallas_call(
        functools.partial(sort_kernel, n),
        in_specs=[pl.BlockSpec(memory_space=pltpu.VMEM)],
        out_specs=pl.BlockSpec(memory_space=pltpu.HBM),
        out_shape=pltpu.HBM((n, cross, share), HALF),
        scratch_shapes=[
            pltpu.VMEM((n, share, cross), HALF),
            pltpu.VMEM((n, cross, share), HALF),
            pltpu.SemaphoreType.DMA((n,)),
        ],
        compiler_params=pltpu.CompilerParams(vmem_limit_bytes=VMEM_LIMIT),
        name="sort_by_owner",
    )(in_vmem(x))


def gram_kernel(chunks, p_hbm, w_hbm, phi_hbm, v_hbm, res_hbm, out_ref, x_ref, *scratch):
    *buffers, left, right, sem = scratch
    sources = (p_hbm, w_hbm, phi_hbm, v_hbm)
    wide = x_ref.shape[1] // chunks
    res_buffer = buffers[-1]
    res_copy = pltpu.make_async_copy(res_hbm, res_buffer, sem.at[len(sources), 0])
    copies = []
    for at in range(chunks):
        cut = pl.ds(at * wide, wide)
        copies.append(
            [
                pltpu.make_async_copy(source.at[:, cut], buffer.at[:, cut], sem.at[i, at])
                for i, (source, buffer) in enumerate(zip(sources, buffers))
            ]
        )
        for copy in copies[-1]:
            copy.start()
        if at == 0:
            res_copy.start()
    for at in range(chunks):
        cut = slice(at * wide, (at + 1) * wide)
        for copy in copies[at]:
            copy.wait()
        if at == 0:
            res_copy.wait()
        p, w, phi, v = [buffer[:, cut].astype(SINGLE) for buffer in buffers[:4]]
        x = jnp.concatenate([p, w], 0).astype(HALF)
        x_ref[:, cut] = x
        more = lax.dot_general(x, x, NT, preferred_element_type=SINGLE)
        left[...] = more if at == 0 else left[...] + more
        y = jnp.concatenate([phi, v], 0).astype(HALF)
        res = res_buffer[cut].astype(SINGLE).reshape(1, wide)
        last = jnp.where(iota((16, wide), 0) == 0, res, 0.0).astype(HALF)
        z = jnp.concatenate([y, last], 0)
        more = lax.dot_general(z, z, NT, preferred_element_type=SINGLE)
        right[...] = more if at == 0 else right[...] + more
    cross = left.shape[0]
    m = LANES
    e = cross - m
    top_right = right[0:m, 0:m]
    same = iota((m, m), 0) == iota((m, m), 1)
    out_ref[0:m, :] = jnp.where(iota((m, m), 1) <= iota((m, m), 0), left[0:m, 0:m], top_right)
    out_ref[m : m + e, :] = left[m:cross, 0:m]
    out_ref[m + e : m + 2 * e, :] = right[m:cross, 0:m]
    corner_right = right[m:cross, m:cross]
    lower = iota((e, e), 1) <= iota((e, e), 0)
    corner = jnp.where(lower, left[m:cross, m:cross], corner_right)
    base = m + 2 * e
    out_ref[base : base + 2 * BLOCK, :] = jnp.zeros((2 * BLOCK, m), SINGLE)
    for i in range(e // BLOCK):
        out_ref[base : base + BLOCK, i * e : (i + 1) * e] = corner[i * BLOCK : (i + 1) * BLOCK, :]
    base += BLOCK
    out_ref[base : base + 1, :] = jnp.sum(jnp.where(same, top_right, 0.0), 0, keepdims=True)
    out_ref[base + 1 : base + 2, :] = right[cross : cross + 1, 0:m]
    out_ref[base + 2 : base + 3, 0 : e + 1] = right[cross : cross + 1, m : cross + 1]
    out_ref[base + 3 : base + 4, 0:e] = jnp.sum(
        jnp.where(iota((e, e), 0) == iota((e, e), 1), corner_right, 0.0), 0, keepdims=True
    )


def packed_rows(cross):
    return LANES + 2 * (cross - LANES) + 2 * BLOCK


def packed_grams(p_left, w_cols, phi_right, v_cols, residual):
    rank, local = p_left.shape
    cols = w_cols.shape[0]
    cross = rank + cols
    chunks = 2
    hbm = pl.BlockSpec(memory_space=pltpu.HBM)
    vmem = pl.BlockSpec(memory_space=pltpu.VMEM)
    return pl.pallas_call(
        functools.partial(gram_kernel, chunks),
        in_specs=[hbm] * 5,
        out_specs=[vmem] * 2,
        out_shape=[
            pltpu.VMEM((packed_rows(cross), LANES), SINGLE),
            pltpu.VMEM((cross, local), HALF),
        ],
        scratch_shapes=[
            pltpu.VMEM((rank, local), HALF),
            pltpu.VMEM((cols, local), HALF),
            pltpu.VMEM((rank, local), HALF),
            pltpu.VMEM((cols, local), HALF),
            pltpu.VMEM((local,), HALF),
            pltpu.VMEM((cross, cross), SINGLE),
            pltpu.VMEM((cross + 16, cross + 16), SINGLE),
            pltpu.SemaphoreType.DMA((5, chunks)),
        ],
        compiler_params=pltpu.CompilerParams(vmem_limit_bytes=VMEM_LIMIT),
        name="packed_grams",
    )(*in_hbm(p_left, w_cols, phi_right, v_cols, residual))


def eliminate(refs, tops):
    crosses = [ref.shape[1] for ref in refs]
    steps = refs[0].shape[0] // BLOCK
    lane, sub = [iota((BLOCK, cross), 1) for cross in crosses], [iota((BLOCK, cross), 0) for cross in crosses]
    thin = iota((BLOCK, 1), 0)

    def step(at, carry):
        row_at = pl.multiple_of(at * BLOCK, BLOCK)
        panels, befores = carry
        for ref, top, x, lanes, cross in zip(refs, tops, befores, lane, crosses):
            far = jnp.where(lanes - (row_at + top) >= BLOCK, x, 0.0)
            r0 = to_half(far)
            r1 = to_half(far - r0)
            r2 = far - r0 - r1
            x0 = to_half(x)
            x1 = to_half(x - x0)
            x2 = x - x0 - x1
            lhs = jnp.concatenate([r0, r0, r0, r1, r1, r2] + [jnp.zeros_like(x)] * 10, 0)
            lhs = lhs.T[top:cross, 0 : 6 * BLOCK].astype(HALF)
            rhs = jnp.concatenate([x0, x1, x2, x0, x1, x0], 0).astype(HALF)
            change = jnp.dot(lhs, rhs, preferred_element_type=SINGLE)
            here = iota(ref.shape, 1) - (row_at + top) + BLOCK
            later = iota(ref.shape, 0) >= row_at + BLOCK
            ref[...] = jnp.where((here >= 0) & (here < BLOCK) & later, 0.0, ref[...]) - change
        columns, scaled = [], []
        for x, top, lanes, subs in zip(panels, tops, lane, sub):
            rel = lanes - (row_at + top)
            columns.append([jnp.sum(jnp.where(rel == i, x, 0.0), 1, keepdims=True) for i in range(BLOCK)])
            scaled.append(jnp.where((rel >= 0) & (rel < BLOCK), jnp.where(rel == subs, 1.0, 0.0), x))
        for i in range(BLOCK):
            for which, column in enumerate(columns):
                scale = lax.rsqrt(column[i][i : i + 1, :])
                factor = jnp.where(thin > i, column[i] * scale, 0.0)
                for j in range(i + 1, BLOCK):
                    column[j] = column[j] - factor * (column[j][i : i + 1, :] * scale)
                x = scaled[which]
                row = x[i : i + 1, :] * scale
                scaled[which] = jnp.where(sub[which] == i, row, x - factor * row)
        nexts = []
        for ref, top, x, lanes, subs in zip(refs, tops, scaled, lane, sub):
            rel = lanes - (row_at + top)
            ref[pl.ds(row_at, BLOCK), :] = jnp.where(rel < BLOCK, x, 0.0)
            ahead = pl.multiple_of(lax.rem(row_at + BLOCK, ref.shape[0]), BLOCK)
            rows = jnp.where((rel >= 0) & (rel < BLOCK), 0.0, ref[pl.ds(ahead, BLOCK), :])
            for i in range(BLOCK):
                row = x[i : i + 1, :]
                weight = jnp.sum(jnp.where(rel == subs + BLOCK, row, 0.0), 1, keepdims=True)
                rows = rows - weight * row
            nexts.append(rows)
        return nexts, scaled

    starts = [ref[0:BLOCK, :] for ref in refs]
    lax.fori_loop(0, steps, step, (starts, [jnp.zeros_like(x) for x in starts]))


def small_kernel(rank, count, g_ref, p_hbm, w_hbm, phi_hbm, v_hbm, *refs):
    top_ref, low_ref, rms_hbm, upd_hbm, q_hbm, left, right, tail, *buffers, norms, update, ready, sem, out_sem = refs
    loads = [
        pltpu.make_async_copy(source, buffer, sem.at[i])
        for i, (source, buffer) in enumerate(zip((p_hbm, w_hbm, phi_hbm, v_hbm), buffers))
    ]
    for load in loads:
        load.start()

    cross = left.shape[0]
    m = LANES
    e = cross - m
    base = m + 2 * e + BLOCK

    def unfold(packed, diagonal):
        rows, lanes = iota(packed.shape, 0), iota(packed.shape, 1)
        lower = jnp.where(lanes < rows, packed, 0.0)
        upper = jnp.where(lanes > rows, packed, 0.0)
        same = rows == lanes
        return (
            lower + lower.T + jnp.where(same, packed, 0.0),
            upper + upper.T + jnp.where(same, diagonal, 0.0),
        )

    left[0:m, 0:m], right[0:m, 0:m] = unfold(g_ref[0:m, :], g_ref[base : base + 1, :])
    left[m:cross, 0:m] = g_ref[m : m + e, :]
    right[m:cross, 0:m] = g_ref[m + e : m + 2 * e, :]
    left[0:m, m:cross] = g_ref[m : m + e, :].T
    right[0:m, m:cross] = g_ref[m + e : m + 2 * e, :].T
    corner = jnp.concatenate(
        [g_ref[base - BLOCK : base, i * e : (i + 1) * e] for i in range(e // BLOCK)], 0
    )
    left[m:cross, m:cross], right[m:cross, m:cross] = unfold(corner, g_ref[base + 3 : base + 4, 0:e])
    g_left = left[...]
    g_right = right[...]
    res_first = g_ref[base + 1 : base + 2, :]
    res_rest = g_ref[base + 2 : base + 3, 0:e]
    res_row = jnp.concatenate([res_first, res_rest], 1)
    res_sq = g_ref[base + 2 : base + 3, e : e + 1]

    tail[...] = g_right[rank:cross, :]
    eliminate([tail], [rank])
    low_lane = iota((cross - rank, cross), 1)
    low_row = iota((cross - rank, cross), 0)
    inverse = jnp.where(low_lane >= rank, tail[...], 0.0)
    eye = jnp.where(iota((rank, cross), 0) == iota((rank, cross), 1), 1.0, 0.0)

    mix = jnp.where(
        low_lane < rank, -to_half(g_right[rank:cross, :]), jnp.where(low_lane == low_row + rank, 1.0, 0.0)
    )
    to_tilde = jnp.concatenate([eye, mix], 0)
    t_right = jnp.concatenate([eye, inverse], 0)
    t_left = jnp.concatenate([eye, dot_hi(inverse, to_tilde)], 0)

    lane8 = iota((BLOCK, cross), 1)
    res8 = jnp.broadcast_to(res_row, (BLOCK, cross))
    half_way = dot_hi(jnp.where(lane8 >= rank, res8, 0.0), inverse, NT)
    coeffs = -dot_hi(half_way, inverse)
    u = dot_hi(jnp.where(lane8 < rank, -to_half(res8), coeffs), to_tilde)
    upd_sq = jnp.sum(dot_hi(u, g_left) * u, 1, keepdims=True)[0:1, :]
    u0 = to_half(u)
    u1 = to_half(u - u0)
    u2 = u - u0 - u1
    sub8 = iota((BLOCK, cross), 0)
    u = jnp.where(sub8 == 0, u0, jnp.where(sub8 == 1, u1, jnp.where(sub8 == 2, u2, 0.0))).astype(HALF)
    norms[...] = jnp.sqrt(jnp.where(iota((1, 2), 1) == 0, res_sq, upd_sq) / count)

    left[...] = dot_hi(dot_hi(t_left, g_left), t_left, NT)
    right[...] = dot_hi(dot_hi(t_right, g_right), t_right, NT)
    eliminate([left, right], [0, 0])
    small = pltpu.make_async_copy(norms, rms_hbm, out_sem.at[out_sem.shape[0] - 1])
    small.start()
    k = dot_hi(left[...], t_left)
    k0 = to_half(k)
    k1 = k - k0
    top_ref[:, 0:m] = k0[0:m, 0:m].astype(HALF)
    top_ref[:, m : 2 * m] = k1[0:m, 0:m].astype(HALF)
    low_ref[0:e, :] = k0[m:cross, :].astype(HALF)
    low_ref[e : 2 * e, :] = k1[m:cross, :].astype(HALF)

    k = dot_hi(right[...], t_right)
    k0 = to_half(k)
    k1 = k - k0
    k_top = jnp.concatenate([k0[0:m, 0:m], k1[0:m, 0:m]], 1).astype(HALF)
    k_low = jnp.concatenate([k0[m:cross], k1[m:cross]], 0).astype(HALF)
    for load in loads:
        load.wait()
    parts = out_sem.shape[0] - 2
    wide = ready.shape[1] // parts
    tile = 256

    def piece(at):
        cut = pl.ds(pl.multiple_of(at * wide, wide), wide)
        return pltpu.make_async_copy(ready.at[:, cut], q_hbm.at[:, cut], out_sem.at[at])

    def multiply(at, carry):
        @pl.when(at > 0)
        def _():
            piece(at - 1).start()

        for to in range(0, wide, tile):
            cut = pl.ds(pl.multiple_of(at * wide + to, tile), tile)
            p, w, phi, v = [buffer[:, cut].astype(SINGLE) for buffer in buffers]
            y = jnp.concatenate([phi, v], 0).astype(HALF)
            twice = jnp.concatenate([y[0:m], y[0:m]], 0)
            ready[0:m, cut] = jnp.dot(k_top, twice, preferred_element_type=SINGLE).astype(HALF)
            low = jnp.dot(k_low, y, preferred_element_type=SINGLE)
            ready[m:cross, cut] = (low[0:e] + low[e : 2 * e]).astype(HALF)
            x = jnp.concatenate([p, w], 0).astype(HALF)
            update[:, cut] = jnp.sum(jnp.dot(u, x, preferred_element_type=SINGLE), 0, keepdims=True)

        return carry

    lax.fori_loop(0, parts, multiply, 0)
    piece(parts - 1).start()
    whole = pltpu.make_async_copy(update, upd_hbm, out_sem.at[parts])
    whole.start()
    for at in range(parts):
        piece(at).wait()
    whole.wait()
    small.wait()


def small_algebra(packed, p_left, w_cols, phi_right, v_cols, count):
    rank, local = p_left.shape
    cols = w_cols.shape[0]
    cross = rank + cols
    parts = 4
    vmem = pl.BlockSpec(memory_space=pltpu.VMEM)
    hbm = pl.BlockSpec(memory_space=pltpu.HBM)
    return pl.pallas_call(
        functools.partial(small_kernel, rank, count),
        in_specs=[vmem] + [hbm] * 4,
        out_specs=[vmem] * 2 + [hbm] * 3,
        out_shape=[
            pltpu.VMEM((LANES, 2 * LANES), HALF),
            pltpu.VMEM((2 * (cross - LANES), cross), HALF),
            pltpu.HBM((1, 2), SINGLE),
            pltpu.HBM((1, local), SINGLE),
            pltpu.HBM((cross, local), HALF),
        ],
        scratch_shapes=[
            pltpu.VMEM((cross, cross), SINGLE),
            pltpu.VMEM((cross, cross), SINGLE),
            pltpu.VMEM((cols, cross), SINGLE),
            pltpu.VMEM((rank, local), HALF),
            pltpu.VMEM((cols, local), HALF),
            pltpu.VMEM((rank, local), HALF),
            pltpu.VMEM((cols, local), HALF),
            pltpu.VMEM((1, 2), SINGLE),
            pltpu.VMEM((1, local), SINGLE),
            pltpu.VMEM((cross, local), HALF),
            pltpu.SemaphoreType.DMA((4,)),
            pltpu.SemaphoreType.DMA((parts + 2,)),
        ],
        compiler_params=pltpu.CompilerParams(vmem_limit_bytes=VMEM_LIMIT),
        name="small_algebra",
    )(in_vmem(packed), *in_hbm(p_left, w_cols, phi_right, v_cols))


def left_kernel(x_ref, top_ref, low_ref, q_ref, ready, sem):
    n, cross, share = x_ref.shape
    m = LANES
    e = cross - m
    group = n // sem.shape[0]
    wide = group * share
    copies = []
    for at in range(sem.shape[0]):
        for i in range(group):
            x = x_ref[at * group + i]
            cut = slice(at * wide + i * share, at * wide + (i + 1) * share)
            twice = jnp.concatenate([x[0:m], x[0:m]], 0)
            ready[0:m, cut] = jnp.dot(top_ref[...], twice, preferred_element_type=SINGLE).astype(HALF)
            low = jnp.dot(low_ref[...], x, preferred_element_type=SINGLE)
            ready[m:cross, cut] = (low[0:e] + low[e : 2 * e]).astype(HALF)
        cut = pl.ds(at * wide, wide)
        copies.append(pltpu.make_async_copy(ready.at[:, cut], q_ref.at[:, cut], sem.at[at]))
        if at:
            copies[-2].start()
    copies[-1].start()
    for copy in copies:
        copy.wait()


def left_products(sorted_x, top, low):
    n, cross, share = sorted_x.shape
    group = max(1, 256 // share)
    vmem = pl.BlockSpec(memory_space=pltpu.VMEM)
    return pl.pallas_call(
        left_kernel,
        in_specs=[vmem, vmem, vmem],
        out_specs=pl.BlockSpec(memory_space=pltpu.HBM),
        out_shape=pltpu.HBM((cross, n * share), HALF),
        scratch_shapes=[
            pltpu.VMEM((cross, n * share), HALF),
            pltpu.SemaphoreType.DMA((n // group,)),
        ],
        compiler_params=pltpu.CompilerParams(vmem_limit_bytes=VMEM_LIMIT),
        name="left_products",
    )(in_vmem(sorted_x), in_vmem(top), in_vmem(low))


def swap(x, reach):
    n = lax.axis_size("rows")
    return lax.ppermute(x, "rows", [(i, i ^ reach) for i in range(n)])


def split(x, reach):
    half = x.shape[0] // 2
    bit = lax.rem(lax.div(lax.axis_index("rows"), reach), 2)
    kept = lax.dynamic_slice_in_dim(x, bit * half, half)
    given = lax.dynamic_slice_in_dim(x, (1 - bit) * half, half)
    return kept + swap(given, reach)


def join(x, reach):
    bit = lax.rem(lax.div(lax.axis_index("rows"), reach), 2)
    other = swap(x, reach)
    return jnp.where(bit == 0, jnp.concatenate([x, other], 0), jnp.concatenate([other, x], 0))


def shards(p_left, phi_right, v_cols, w_cols, residual):
    _, local = p_left.shape
    n = lax.axis_size("rows")
    near = [1 << i for i in range(3)]
    far = [1 << i for i in range(3, n.bit_length() - 1)]
    packed, x = packed_grams(p_left, w_cols, phi_right, v_cols, residual)
    mine = sort_by_owner(x, n)
    other = swap(packed, far[-1])
    owned = lax.all_to_all(mine, "rows", split_axis=0, concat_axis=0, tiled=True)
    packed = packed + other
    packed = split(packed, near[0])
    for reach in near[1:]:
        packed = packed + swap(packed, reach)
    for reach in far[:-1]:
        packed = packed + swap(packed, reach)
    packed = join(packed, near[0])
    k_top, k_low, rms, update, q_right = small_algebra(
        packed, p_left, w_cols, phi_right, v_cols, float(local * n)
    )
    q_left = left_products(owned, k_top, k_low)
    return (update.reshape(local), q_left, q_right, rms.reshape(2))


def solution(mesh):
    placed = (P(None, "rows"), P(None, "rows"), P(None, "rows"), P(None, "rows"), P("rows"))
    return jax.shard_map(
        shards,
        mesh=mesh,
        in_specs=placed,
        out_specs=(P("rows"), P(None, "rows"), P(None, "rows"), P()),
        check_vma=False,
    )
```
